32 devices in a mesh: rep: 4 (over x, core), mx: 2 (over y), my: 4 (over z).
Axes of the slice: x: 2, y: 2, z: 4, core: 2. Of those that a mesh axis runs over, the one named last changes fastest.
Arguments:
- coefficients: bfloat16 [2, 384, 384, 384], P(None, 'mx', 'my'), may hold values from -7.5 to 7.5
- noise_field: bfloat16 [128, 2, 1536, 1536], P(('rep', 'mx'), None, 'my'), may hold values from -96 to 96
- mode_table: bfloat16 [384, 1536], replicated, may hold values from -0.3125 to 0.3125
Outputs:
- update: bfloat16 [2, 384, 384, 384], P(None, 'mx', 'my', 'rep')
The draws below stay inside these ranges and needn't reach their ends.
All inputs are finite; a program needn't handle non-finite values.
Results may differ from the reference program's by a relative error of at most 0.008.
Values may be sent and summed in bfloat16 or wider, within the bound.
A program may use at most 384 MiB of HBM per device.

```python
import jax
import jax.numpy as jnp
from jax import lax

MODES = 384
POINTS = 1536
PLANES = 128


def steps_of(own_key, extent, pieces, smallest, largest):
    gain, own = 1.0, jax.random.fold_in(own_key, 6)
    for axis_at, shards_of in pieces:
        heights = jnp.exp(jax.random.uniform(jax.random.fold_in(own, axis_at), (shards_of,), jnp.float32, smallest / len(pieces), largest / len(pieces)))
        gain = gain * jnp.repeat(heights, extent[axis_at] // shards_of).reshape([-1 if axis == axis_at else 1 for axis in range(len(extent))])
    return gain


def normal_values(key, dims, scale, bound, cuts=(), dtype=jnp.bfloat16):
    values = scale * jax.random.normal(key, dims, jnp.float32)
    if cuts:
        values = values * steps_of(key, dims, cuts, -0.22, 0.18)
    return jnp.clip(values, -bound, bound).astype(dtype)


def setup_inputs(seed: int = 0) -> dict:
    key_list = jax.random.split(jax.random.key(seed), 4)
    return {
        "coefficients": normal_values(key_list[0], (2, MODES, MODES, MODES), 1.25, 7.5, ((1, 2), (2, 4))),
        "noise_field": normal_values(key_list[1], (PLANES, 2, POINTS, POINTS), 16.0, 96.0, ((0, 8), (2, 4))),
        "mode_table": normal_values(key_list[2], (MODES, POINTS), MODES ** -0.5, 0.3125),
    }


DAMPING = 0.25


def reference(coefficients, noise_field, mode_table):
    slab_first = POINTS // 2 - PLANES // 2
    table_wide = mode_table.astype(jnp.float32)
    slab_table = table_wide[:, slab_first:slab_first + PLANES]
    zmodes = jnp.einsum('pabk,kz->zpab', coefficients.astype(jnp.float32), slab_table).astype(jnp.bfloat16)

    def one_plane(inputs):
        plane_modes, plane_noise = inputs
        xmodes = jnp.einsum('pab,ax->pbx', plane_modes.astype(jnp.float32), table_wide).astype(jnp.bfloat16)
        wave_field = jnp.einsum('pbx,by->pxy', xmodes.astype(jnp.float32), table_wide)
        wave_real = wave_field[0]
        wave_imag = wave_field[1]
        density = wave_real * wave_real + wave_imag * wave_imag
        noise_wide = plane_noise.astype(jnp.float32)
        drive_term = jnp.stack([density * (wave_imag - DAMPING * wave_real) + noise_wide[0],
                                density * (-wave_real - DAMPING * wave_imag) + noise_wide[1]], 0).astype(jnp.bfloat16)
        proj_columns = jnp.einsum('pxy,by->pbx', drive_term.astype(jnp.float32), table_wide).astype(jnp.bfloat16)
        proj_rows = jnp.einsum('pbx,ax->pab', proj_columns.astype(jnp.float32), table_wide).astype(jnp.bfloat16)
        return proj_rows

    projected = lax.map(one_plane, (zmodes, noise_field))
    update = jnp.einsum('zpab,nz->pabn', projected.astype(jnp.float32), slab_table)
    return update.astype(jnp.bfloat16)
```

```python
import jax
import jax.numpy as jnp
from jax import lax
from jax.experimental import pallas as pl
from jax.experimental.pallas import tpu as pltpu
from jax.sharding import PartitionSpec as P

DAMPING = 0.25
MESH = pl.DeviceIdType.MESH
NT = (((1,), (1,)), ((), ()))


def plain_body(coefficients, noise_field, mode_table):
    rep_index = lax.axis_index("rep")
    col_index = lax.axis_index("my")
    rep_count = lax.axis_size("rep")
    row_count = lax.axis_size("mx")
    col_count = lax.axis_size("my")
    planes_dev = noise_field.shape[0]
    planes_rep = planes_dev * row_count
    planes_all = planes_rep * rep_count
    mode_count = mode_table.shape[0]
    point_count = mode_table.shape[1]
    slab_first = point_count // 2 - planes_all // 2
    row_block = mode_count // row_count
    col_block = mode_count // col_count
    point_block = point_count // col_count
    own_block = mode_count // rep_count
    slab_own = lax.dynamic_slice_in_dim(
        mode_table, slab_first + rep_index * planes_rep, planes_rep, 1
    )
    zmodes = jnp.einsum(
        "pabk,kz->zpba", coefficients, slab_own, preferred_element_type=jnp.float32
    ).astype(jnp.bfloat16)
    zmodes = zmodes.reshape(planes_rep, 2, col_block * row_block)
    spread = lax.all_to_all(zmodes, "mx", split_axis=0, concat_axis=2, tiled=True)
    grouped = spread.reshape(planes_dev, 2, row_count, col_block, row_block)
    tiled_table = mode_table.reshape(row_count, row_block, point_count)
    own_points = lax.dynamic_slice_in_dim(tiled_table, col_index * point_block, point_block, 2)
    block_part = jnp.einsum(
        "zpsal,slx->zpax",
        lax.all_gather(grouped, "my", axis=3, tiled=True),
        own_points,
        preferred_element_type=jnp.float32,
    ).astype(jnp.bfloat16)
    wave_field = jnp.einsum(
        "zpax,ay->zpxy", block_part, mode_table, preferred_element_type=jnp.float32
    )
    wave_real = wave_field[:, 0]
    wave_imag = wave_field[:, 1]
    density = wave_real * wave_real + wave_imag * wave_imag
    noise_wide = noise_field.astype(jnp.float32)
    drive_term = jnp.stack(
        [
            density * (wave_imag - DAMPING * wave_real) + noise_wide[:, 0],
            density * (-wave_real - DAMPING * wave_imag) + noise_wide[:, 1],
        ],
        1,
    ).astype(jnp.bfloat16)
    proj_columns = jnp.einsum(
        "zpxy,ny->zpnx", drive_term, mode_table, preferred_element_type=jnp.float32
    ).astype(jnp.bfloat16)
    block_part = lax.all_to_all(proj_columns, "my", split_axis=2, concat_axis=3, tiled=True)
    folded = jnp.einsum(
        "zpax,slx->zpsal", block_part, tiled_table, preferred_element_type=jnp.float32
    ).astype(jnp.bfloat16)
    proj_rows = folded.reshape(
        block_part.shape[0], block_part.shape[1], row_count * col_block * row_block
    )
    gathered_rows = lax.all_to_all(proj_rows, "mx", split_axis=2, concat_axis=0, tiled=True)
    slab_back = lax.dynamic_slice_in_dim(mode_table, rep_index * own_block, own_block, 0)[
        :, slab_first : slab_first + planes_all
    ]
    portion = lax.all_gather(gathered_rows, "rep", axis=0, tiled=True)
    plane_grid = portion.reshape(portion.shape[0], 2, col_block, row_block)
    summed = jnp.einsum("zpba,nz->pabn", plane_grid, slab_back, preferred_element_type=jnp.float32)
    return summed.astype(jnp.bfloat16)

def slab_schedule(planes, count, units):
    half = count // 2
    per = planes // count

    def first_of(me):
        group = me - half if me >= half else half - 1 - me
        return group * 2 * per + (1 if me >= half else 0)

    def needed(me):
        return max((k + 1) * units - first_of(me) - 2 * k for k in range(per))

    lag_end = max(0, needed(0), needed(count - 1))
    lag_mid = max([lag_end + 1] + [needed(me) for me in range(1, count - 1)])
    return half, per, lag_end, lag_mid


def slab_kernel(own_ref, noise_ref, table_ref, turned_ref, out_ref, modes, lines, total, cubic, parts,
                landed, noise, halves, noise_sem, mode_recv, mode_send, sum_recv, sum_send, last_recv,
                last_send):
    count = lax.axis_size("my")
    me = lax.axis_index("my")
    row_count = lax.axis_size("mx")
    row = lax.axis_index("mx")
    rep_count = lax.axis_size("rep")
    rep = lax.axis_index("rep")
    planes = own_ref.shape[0] // row_count
    block = own_ref.shape[2]
    row_block = own_ref.shape[3]
    offsets = [(dr, dh) for dr in range(rep_count) for dh in range(row_count)]
    mode_count, point_count = table_ref.shape
    point_block = noise_ref.shape[2]
    width = lines.shape[1] // 2
    units = point_count // width
    chunk = 256 if point_count % 256 == 0 else 128
    half, per, lag_end, lag_mid = slab_schedule(planes, count, units)
    up = {"my": me + 1}
    down = {"my": me - 1}
    has_up = me < count - 1
    has_down = me > 0

    barrier = pltpu.get_barrier_semaphore()
    line_peers = [(dh, dm) for dh in range(row_count) for dm in range(count)][1:]
    rep_peers = [(dr, dh) for dr, dh in offsets if dr > 0]
    for dh, dm in line_peers:
        pl.semaphore_signal(
            barrier, inc=1,
            device_id={"mx": lax.rem(row + dh, row_count), "my": lax.rem(me + dm, count)},
            device_id_type=MESH,
        )
    for dr, dh in rep_peers:
        pl.semaphore_signal(
            barrier, inc=1,
            device_id={"rep": lax.rem(rep + dr, rep_count), "mx": lax.rem(row + dh, row_count)},
            device_id_type=MESH,
        )

    def rows(j):
        return pl.ds(pl.multiple_of(j * block, block), block)

    def owner_of(p):
        group = lax.div(p, 2 * per)
        return jnp.where(lax.rem(p, 2) == 1, half + group, half - 1 - group)

    def slot_of(p):
        return lax.div(lax.rem(p, 2 * per), 2)

    def plane_of(k):
        group = jnp.where(me >= half, me - half, half - 1 - me)
        return group * (2 * per) + 2 * k + (me >= half).astype(jnp.int32)

    def mode_copy(p, h, j, target_row, target):
        return pltpu.make_async_remote_copy(
            src_ref=own_ref.at[target_row * planes + p],
            dst_ref=modes.at[slot_of(p), h, :, rows(j)],
            send_sem=mode_send.at[p, target_row],
            recv_sem=mode_recv.at[slot_of(p), h, j],
            device_id={"mx": target_row, "my": target},
            device_id_type=MESH,
        )

    def mode_keep(p):
        return pltpu.make_async_copy(
            own_ref.at[row * planes + p], modes.at[slot_of(p), row, :, rows(me)],
            mode_recv.at[slot_of(p), row, me],
        )

    def last_copy(p, at, received):
        dr, dh = offsets[at]
        target = lax.rem(row + dh, row_count)
        if received:
            from_rep = lax.rem(rep + rep_count - dr, rep_count)
            from_row = lax.rem(row + row_count - dh, row_count)
        else:
            from_rep, from_row = rep, row
        plane = (from_rep * row_count + from_row) * planes + p
        if at == 0:
            return pltpu.make_async_copy(halves.at[p, row], out_ref.at[plane], last_send.at[p, 0])
        return pltpu.make_async_remote_copy(
            src_ref=halves.at[p, target],
            dst_ref=out_ref.at[plane],
            send_sem=last_send.at[p, at],
            recv_sem=last_recv.at[p, at],
            device_id={"rep": lax.rem(rep + dr, rep_count), "mx": target},
            device_id_type=MESH,
        )

    def noise_copy(p):
        slot = lax.rem(p, 2)
        return pltpu.make_async_copy(noise_ref.at[p], noise.at[slot], noise_sem.at[slot])

    def sum_copy(p, j, way, slot):
        return pltpu.make_async_remote_copy(
            src_ref=parts.at[p, :, rows(j)],
            dst_ref=landed.at[p, slot],
            send_sem=sum_send.at[p, way, j],
            recv_sem=sum_recv.at[p, slot],
            device_id=down if way else up,
            device_id_type=MESH,
        )

    noise_copy(0).start()
    if planes > 1:
        noise_copy(1).start()

    pl.semaphore_wait(barrier, len(line_peers) + len(rep_peers))

    def send_modes(p, carry):
        target = owner_of(p)
        for dh in range(row_count):
            target_row = lax.rem(row + dh, row_count)
            if dh:
                mode_copy(p, row, me, target_row, target).start()
            else:
                @pl.when(target != me)
                def _():
                    mode_copy(p, row, me, target_row, target).start()

                @pl.when(target == me)
                def _():
                    mode_keep(p).start()
        return carry

    lax.fori_loop(0, planes, send_modes, 0)

    def inside(p):
        return jnp.logical_and(p >= 0, p < planes)

    own_points = pl.ds(pl.multiple_of(me * point_block, point_block), point_block)

    def project_noise(p):
        noise_copy(p).wait()
        slot = lax.rem(p, 2)
        step_of = max(c for c in (512, 256, 128) if point_count % c == 0)
        columns = None
        for first in range(0, point_count, step_of):
            span = slice(first, first + step_of)
            field = noise[slot, :, :, span].reshape(2 * point_block, step_of)
            more = lax.dot_general(table_ref[:, span], field, NT, preferred_element_type=jnp.float32)
            columns = more if columns is None else columns + more
        turned = turned_ref[own_points]
        for part in range(2):
            column = columns[:, part * point_block : (part + 1) * point_block].astype(jnp.bfloat16)
            parts[p, part] = jnp.dot(column, turned, preferred_element_type=jnp.float32).astype(
                jnp.bfloat16
            )

        @pl.when(p + 2 < planes)
        def _():
            noise_copy(p + 2).start()

    def wait_modes(k):
        p = plane_of(k)
        for h in range(row_count):
            for j in range(count):
                mine = jnp.logical_and(row == h, me == j)

                @pl.when(mine)
                def _():
                    mode_keep(p).wait()

                @pl.when(jnp.logical_not(mine))
                def _():
                    mode_copy(p, h, j, row, me).wait_recv()

    def cubic_unit(u):
        k = lax.div(u, units)
        at = lax.rem(u, units)

        @pl.when(at == 0)
        def _():
            wait_modes(k)

        span = pl.ds(pl.multiple_of(at * width, width), width)
        for part in range(2):
            line = None
            for h in range(row_count):
                more = jnp.dot(
                    modes[k, h, part], table_ref[h * row_block : (h + 1) * row_block, span],
                    preferred_element_type=jnp.float32,
                )
                line = more if line is None else line + more
            lines[:, part * width : (part + 1) * width] = line.astype(jnp.bfloat16)
        columns = None
        for first in range(0, point_count, chunk):
            wave = jnp.dot(
                turned_ref[first : first + chunk], lines[...], preferred_element_type=jnp.float32
            )
            wave_real, wave_imag = wave[:, :width], wave[:, width:]
            density = wave_real * wave_real + wave_imag * wave_imag
            drive = jnp.concatenate(
                [
                    (density * (wave_imag - DAMPING * wave_real)).astype(jnp.bfloat16),
                    (density * (-wave_real - DAMPING * wave_imag)).astype(jnp.bfloat16),
                ],
                1,
            )
            more = jnp.dot(
                table_ref[:, first : first + chunk], drive, preferred_element_type=jnp.float32
            )
            columns = more if columns is None else columns + more
        for part in range(2):
            more = jnp.dot(
                columns[:, part * width : (part + 1) * width].astype(jnp.bfloat16),
                turned_ref[span], preferred_element_type=jnp.float32,
            )

            @pl.when(at == 0)
            def _():
                total[part] = more

            @pl.when(at > 0)
            def _():
                total[part] += more

        @pl.when(at == units - 1)
        def _():
            cubic[k] = total[...].astype(jnp.bfloat16)

    def add(p, j, slot):
        wide = parts[p, :, rows(j)].astype(jnp.float32) + landed[p, slot].astype(jnp.float32)
        parts[p, :, rows(j)] = wide.astype(jnp.bfloat16)

    rise_lag = jnp.where(me == 0, lag_end, lag_mid + me - 1)
    sink_lag = jnp.where(me == count - 1, lag_end, lag_mid + count - 2 - me)
    merge_lag = jnp.minimum(rise_lag, sink_lag)
    done_lag = jnp.maximum(rise_lag, sink_lag)

    def step(s, carry):
        @pl.when(s < planes)
        def _():
            project_noise(s)

        merging = s - merge_lag

        @pl.when(jnp.logical_and(inside(merging), owner_of(merging) == me))
        def _():
            wide = parts[merging].astype(jnp.float32) + cubic[slot_of(merging)].astype(jnp.float32)
            parts[merging] = wide.astype(jnp.bfloat16)

        rising = s - rise_lag
        sinking = s - sink_lag

        @pl.when(jnp.logical_and(inside(rising), me == 0))
        def _():
            for j in range(count - 1, 0, -1):
                sum_copy(rising, j, 0, j).start()

        @pl.when(jnp.logical_and(inside(sinking), me == count - 1))
        def _():
            for j in range(count - 1):
                sum_copy(sinking, j, 1, count if j == count - 2 else j).start()

        @pl.when(s < per * units)
        def _():
            cubic_unit(s)

        for far in range(count - 2, 0, -1):
            @pl.when(jnp.logical_and(jnp.logical_and(inside(rising), has_down), me + far <= count - 1))
            def _():
                j = me + far
                sum_copy(rising, j, 0, j).wait_recv()
                add(rising, j, j)
                sum_copy(rising, j, 0, j).start()

        for far in range(count - 2, 0, -1):
            @pl.when(jnp.logical_and(jnp.logical_and(inside(sinking), has_up), me - far >= 0))
            def _():
                j = me - far
                sum_copy(sinking, j, 1, j).wait_recv()
                add(sinking, j, j)
                sum_copy(sinking, j, 1, count if far == 1 else j).start()

        done = s - done_lag

        @pl.when(inside(done))
        def _():
            @pl.when(has_down)
            def _():
                sum_copy(done, me, 0, me).wait_recv()
                add(done, me, me)

            @pl.when(has_up)
            def _():
                sum_copy(done, me, 1, count).wait_recv()
                add(done, me, count)

            for part in range(2):
                whole = parts[done, part, rows(me)]
                for h in range(row_count):
                    halves[done, h, part] = whole[:, h * row_block : (h + 1) * row_block]
            for at in range(len(offsets)):
                last_copy(done, at, False).start()

        return carry

    lax.fori_loop(0, planes + lag_mid + count - 2, step, 0)

    def finish(p, carry):
        for j in range(count):
            @pl.when(j > me)
            def _():
                sum_copy(p, j, 0, j).wait_send()

            @pl.when(j < me)
            def _():
                sum_copy(p, j, 1, j).wait_send()

        target = owner_of(p)
        for dh in range(row_count):
            target_row = lax.rem(row + dh, row_count)
            if dh:
                mode_copy(p, row, me, target_row, target).wait_send()
            else:
                @pl.when(target != me)
                def _():
                    mode_copy(p, row, me, target_row, target).wait_send()

        last_copy(p, 0, False).wait()
        for at in range(1, len(offsets)):
            last_copy(p, at, False).wait_send()
            last_copy(p, at, True).wait_recv()
        return carry

    lax.fori_loop(0, planes, finish, 0)


def slab_planes(own_modes, noise_field, mode_table, turned):
    count = lax.axis_size("my")
    mode_count = mode_table.shape[0]
    row_count = lax.axis_size("mx")
    rep_count = lax.axis_size("rep")
    planes_rep, _, block, row_block = own_modes.shape
    planes = planes_rep // row_count
    per = planes // count
    point_block, point_count = noise_field.shape[2:]
    width = max(c for c in (512, 256, 128) if point_count % c == 0)
    vmem = pl.BlockSpec(memory_space=pltpu.VMEM)
    hbm = pl.BlockSpec(memory_space=pl.ANY)
    dma = pltpu.SemaphoreType.DMA
    flops = 12 * planes * mode_count * point_block * (point_count + mode_count)
    return pl.pallas_call(
        slab_kernel,
        out_shape=jax.ShapeDtypeStruct((planes_rep * rep_count, 2, block, row_block), jnp.bfloat16),
        in_specs=[hbm, hbm, vmem, vmem],
        out_specs=hbm,
        scratch_shapes=[
            pltpu.VMEM((per, row_count, 2, mode_count, row_block), jnp.bfloat16),
            pltpu.VMEM((mode_count, 2 * width), jnp.bfloat16),
            pltpu.VMEM((2, mode_count, mode_count), jnp.float32),
            pltpu.VMEM((per, 2, mode_count, mode_count), jnp.bfloat16),
            pltpu.VMEM((planes, 2, mode_count, mode_count), jnp.bfloat16),
            pltpu.VMEM((planes, count + 1, 2, block, mode_count), jnp.bfloat16),
            pltpu.VMEM((2, 2, point_block, point_count), jnp.bfloat16),
            pltpu.VMEM((planes, row_count, 2, block, row_block), jnp.bfloat16),
            dma((2,)),
            dma((per, row_count, count)),
            dma((planes, row_count)),
            dma((planes, count + 1)),
            dma((planes, 2, count)),
            dma((planes, row_count * rep_count)),
            dma((planes, row_count * rep_count)),
        ],
        compiler_params=pltpu.CompilerParams(
            collective_id=0, has_side_effects=True, vmem_limit_bytes=60 * 1024 * 1024
        ),
        cost_estimate=pl.CostEstimate(
            flops=flops, bytes_accessed=noise_field.size * 2, transcendentals=0
        ),
    )(own_modes, noise_field, mode_table, turned)


def body(coefficients, noise_field, mode_table):
    rep_index = lax.axis_index("rep")
    rep_count = lax.axis_size("rep")
    row_count = lax.axis_size("mx")
    col_count = lax.axis_size("my")
    planes_dev = noise_field.shape[0]
    planes_rep = planes_dev * row_count
    planes_all = planes_rep * rep_count
    mode_count = mode_table.shape[0]
    point_count = mode_table.shape[1]
    slab_first = point_count // 2 - planes_all // 2
    row_block = mode_count // row_count
    col_block = mode_count // col_count
    point_block = point_count // col_count
    own_block = mode_count // rep_count
    if (
        col_block % 16 or row_block % 16 or point_block % 128 or mode_count % 128
        or col_count < 2 or col_count % 2 or planes_dev % col_count
    ):
        return plain_body(coefficients, noise_field, mode_table)
    slab_own = lax.dynamic_slice_in_dim(
        mode_table, slab_first + rep_index * planes_rep, planes_rep, 1
    )
    zmodes = jnp.einsum(
        "pabk,kz->zpba", coefficients, slab_own, preferred_element_type=jnp.float32
    ).astype(jnp.bfloat16)
    plane_grid = slab_planes(zmodes, noise_field, mode_table, mode_table.T)
    slab_back = lax.dynamic_slice_in_dim(mode_table, rep_index * own_block, own_block, 0)[
        :, slab_first : slab_first + planes_all
    ]
    summed = jnp.einsum("zpba,nz->pabn", plane_grid, slab_back, preferred_element_type=jnp.float32)
    return summed.astype(jnp.bfloat16)


def solution(mesh):
    in_specs = (P(None, "mx", "my", None), P(("rep", "mx"), None, "my", None), P())
    out_specs = P(None, "mx", "my", "rep")
    return jax.shard_map(body, mesh=mesh, in_specs=in_specs, out_specs=out_specs, check_vma=False)
```

```python
import jax
import jax.numpy as jnp
from jax import lax
from jax.experimental import pallas as pl
from jax.experimental.pallas import tpu as pltpu
from jax.sharding import PartitionSpec as P

DAMPING = 0.25
MESH = pl.DeviceIdType.MESH
NT = (((1,), (1,)), ((), ()))


def plain_body(coefficients, noise_field, mode_table):
    rep_index = lax.axis_index("rep")
    col_index = lax.axis_index("my")
    rep_count = lax.axis_size("rep")
    row_count = lax.axis_size("mx")
    col_count = lax.axis_size("my")
    planes_dev = noise_field.shape[0]
    planes_rep = planes_dev * row_count
    planes_all = planes_rep * rep_count
    mode_count = mode_table.shape[0]
    point_count = mode_table.shape[1]
    slab_first = point_count // 2 - planes_all // 2
    row_block = mode_count // row_count
    col_block = mode_count // col_count
    point_block = point_count // col_count
    own_block = mode_count // rep_count
    slab_own = lax.dynamic_slice_in_dim(
        mode_table, slab_first + rep_index * planes_rep, planes_rep, 1
    )
    zmodes = jnp.einsum(
        "pabk,kz->zpba", coefficients, slab_own, preferred_element_type=jnp.float32
    ).astype(jnp.bfloat16)
    zmodes = zmodes.reshape(planes_rep, 2, col_block * row_block)
    spread = lax.all_to_all(zmodes, "mx", split_axis=0, concat_axis=2, tiled=True)
    grouped = spread.reshape(planes_dev, 2, row_count, col_block, row_block)
    tiled_table = mode_table.reshape(row_count, row_block, point_count)
    own_points = lax.dynamic_slice_in_dim(tiled_table, col_index * point_block, point_block, 2)
    block_part = jnp.einsum(
        "zpsal,slx->zpax",
        lax.all_gather(grouped, "my", axis=3, tiled=True),
        own_points,
        preferred_element_type=jnp.float32,
    ).astype(jnp.bfloat16)
    wave_field = jnp.einsum(
        "zpax,ay->zpxy", block_part, mode_table, preferred_element_type=jnp.float32
    )
    wave_real = wave_field[:, 0]
    wave_imag = wave_field[:, 1]
    density = wave_real * wave_real + wave_imag * wave_imag
    noise_wide = noise_field.astype(jnp.float32)
    drive_term = jnp.stack(
        [
            density * (wave_imag - DAMPING * wave_real) + noise_wide[:, 0],
            density * (-wave_real - DAMPING * wave_imag) + noise_wide[:, 1],
        ],
        1,
    ).astype(jnp.bfloat16)
    proj_columns = jnp.einsum(
        "zpxy,ny->zpnx", drive_term, mode_table, preferred_element_type=jnp.float32
    ).astype(jnp.bfloat16)
    block_part = lax.all_to_all(proj_columns, "my", split_axis=2, concat_axis=3, tiled=True)
    folded = jnp.einsum(
        "zpax,slx->zpsal", block_part, tiled_table, preferred_element_type=jnp.float32
    ).astype(jnp.bfloat16)
    proj_rows = folded.reshape(
        block_part.shape[0], block_part.shape[1], row_count * col_block * row_block
    )
    gathered_rows = lax.all_to_all(proj_rows, "mx", split_axis=2, concat_axis=0, tiled=True)
    slab_back = lax.dynamic_slice_in_dim(mode_table, rep_index * own_block, own_block, 0)[
        :, slab_first : slab_first + planes_all
    ]
    portion = lax.all_gather(gathered_rows, "rep", axis=0, tiled=True)
    plane_grid = portion.reshape(portion.shape[0], 2, col_block, row_block)
    summed = jnp.einsum("zpba,nz->pabn", plane_grid, slab_back, preferred_element_type=jnp.float32)
    return summed.astype(jnp.bfloat16)

def slab_schedule(planes, count, units, rate, first_step):
    half = count // 2
    per = planes // count

    def first_of(me):
        group = me - half if me >= half else half - 1 - me
        return group * 2 * per + (1 if me >= half else 0)

    def needed(me):
        ready = [first_step + ((k + 1) * units - 1) // rate for k in range(per)]
        return max(ready[k] + 1 - first_of(me) - 2 * k for k in range(per))

    lag_end = max(0, needed(0), needed(count - 1))
    lag_mid = max([lag_end + 1] + [needed(me) for me in range(1, count - 1)])
    return half, per, lag_end, lag_mid


def slab_kernel(coef_ref, noise_ref, table_ref, turned_ref, slab_ref, out_ref, coef, wide, spread, zmodes,
                modes, lines, total, cubic, parts, landed, noise, halves, coef_sem, noise_sem, mode_recv,
                mode_send, sum_recv, sum_send, first_recv, first_send, second_recv, second_send):
    count = lax.axis_size("my")
    me = lax.axis_index("my")
    row_count = lax.axis_size("mx")
    row = lax.axis_index("mx")
    rep_count = lax.axis_size("rep")
    rep = lax.axis_index("rep")
    planes = noise_ref.shape[0]
    planes_rep = planes * row_count
    row_block = coef_ref.shape[1]
    block = coef_ref.shape[2]
    pair = 2 if rep_count % 2 == 0 else 1
    groups = rep_count // pair
    group = lax.div(rep, pair)
    side = lax.rem(rep, pair)
    spots = [(dg, dh) for dg in range(groups) for dh in range(row_count)]
    offsets = [(dr, dh) for dr in range(rep_count) for dh in range(row_count)]
    tiles = [(t, first, min(128, row_block - first)) for t, first in enumerate(range(0, row_block, 128))]
    mode_count, point_count = table_ref.shape
    point_block = noise_ref.shape[2]
    width = lines.shape[1] // 2
    units = point_count // width
    chunk = 256 if point_count % 256 == 0 else 128
    rate = max(1, units // 2)
    modes_step, cubic_step = 2, 4
    half, per, lag_end, lag_mid = slab_schedule(planes, count, units, rate, cubic_step)
    up = {"my": me + 1}
    down = {"my": me - 1}
    has_up = me < count - 1
    has_down = me > 0

    barrier = pltpu.get_barrier_semaphore()
    line_peers = [(dh, dm) for dh in range(row_count) for dm in range(count)][1:]
    rep_peers = [(dr, dh) for dr, dh in offsets if dr > 0]
    for dh, dm in line_peers:
        pl.semaphore_signal(
            barrier, inc=1,
            device_id={"mx": lax.rem(row + dh, row_count), "my": lax.rem(me + dm, count)},
            device_id_type=MESH,
        )
    for dr, dh in rep_peers:
        pl.semaphore_signal(
            barrier, inc=1,
            device_id={"rep": lax.rem(rep + dr, rep_count), "mx": lax.rem(row + dh, row_count)},
            device_id_type=MESH,
        )

    def rows(j):
        return pl.ds(pl.multiple_of(j * block, block), block)

    def owner_of(p):
        group = lax.div(p, 2 * per)
        return jnp.where(lax.rem(p, 2) == 1, half + group, half - 1 - group)

    def slot_of(p):
        return lax.div(lax.rem(p, 2 * per), 2)

    def plane_of(k):
        group = jnp.where(me >= half, me - half, half - 1 - me)
        return group * (2 * per) + 2 * k + (me >= half).astype(jnp.int32)

    def mode_copy(p, h, j, target_row, target):
        return pltpu.make_async_remote_copy(
            src_ref=zmodes.at[target_row * planes + p],
            dst_ref=modes.at[slot_of(p), h, :, rows(j)],
            send_sem=mode_send.at[p, target_row],
            recv_sem=mode_recv.at[slot_of(p), h, j],
            device_id={"mx": target_row, "my": target},
            device_id_type=MESH,
        )

    def mode_keep(p):
        return pltpu.make_async_copy(
            zmodes.at[row * planes + p], modes.at[slot_of(p), row, :, rows(me)],
            mode_recv.at[slot_of(p), row, me],
        )

    def plane_at(from_group, from_side, from_row, p):
        return ((from_group * pair + from_side) * row_count + from_row) * planes + p

    def first_copy(p, at, received):
        dg, dh = spots[at]
        target_row = lax.rem(row + dh, row_count)
        if at == 0:
            return pltpu.make_async_copy(
                halves.at[p, row], out_ref.at[plane_at(group, side, row, p)], first_send.at[p, 0]
            )
        if received:
            plane = plane_at(
                lax.rem(group + groups - dg, groups), side, lax.rem(row + row_count - dh, row_count), p
            )
        else:
            plane = plane_at(group, side, row, p)
        return pltpu.make_async_remote_copy(
            src_ref=halves.at[p, target_row],
            dst_ref=out_ref.at[plane],
            send_sem=first_send.at[p, at],
            recv_sem=first_recv.at[p, at],
            device_id={"rep": lax.rem(group + dg, groups) * pair + side, "mx": target_row},
            device_id_type=MESH,
        )

    def second_copy(p, at, received):
        dg, dh = spots[at]
        plane = plane_at(
            lax.rem(group + groups - dg, groups), 1 - side if received else side,
            lax.rem(row + row_count - dh, row_count), p,
        )
        return pltpu.make_async_remote_copy(
            src_ref=halves.at[p, row] if at == 0 else out_ref.at[plane],
            dst_ref=out_ref.at[plane],
            send_sem=second_send.at[p, at],
            recv_sem=second_recv.at[p, at],
            device_id={"rep": group * pair + 1 - side},
            device_id_type=MESH,
        )

    def noise_copy(p):
        slot = lax.rem(p, 2)
        return pltpu.make_async_copy(noise_ref.at[p], noise.at[slot], noise_sem.at[slot])

    def sum_copy(p, j, way, slot):
        return pltpu.make_async_remote_copy(
            src_ref=parts.at[p, :, rows(j)],
            dst_ref=landed.at[p, slot],
            send_sem=sum_send.at[p, way, j],
            recv_sem=sum_recv.at[p, slot],
            device_id=down if way else up,
            device_id_type=MESH,
        )

    strips = block // 16

    def coef_copy(i):
        slot = lax.rem(i, 2)
        strip = pl.ds(pl.multiple_of(lax.rem(i, strips) * 16, 16), 16)
        return pltpu.make_async_copy(
            coef_ref.at[lax.div(i, strips), :, strip], coef.at[slot], coef_sem.at[slot]
        )

    noise_copy(0).start()
    if planes > 1:
        noise_copy(1).start()
    coef_copy(0).start()
    coef_copy(1).start()

    pl.semaphore_wait(barrier, len(line_peers) + len(rep_peers))

    def contract_strip(i, carry):
        coef_copy(i).wait()
        part = lax.div(i, strips)
        strip = pl.ds(pl.multiple_of(lax.rem(i, strips) * 16, 16), 16)
        wide[...] = jnp.dot(
            coef[lax.rem(i, 2)].reshape(row_block * 16, coef.shape[3]), slab_ref[...],
            preferred_element_type=jnp.float32,
        )

        @pl.when(i + 2 < 2 * strips)
        def _():
            coef_copy(i + 2).start()

        for b in range(16):
            for t, first, size in tiles:
                turn = wide[pl.ds(first * 16 + b, size, stride=16), :].T[:planes_rep]
                if size < 128:
                    turn = jnp.concatenate([turn, jnp.zeros((planes_rep, 128 - size), jnp.float32)], 1)
                spread[t, pl.ds(b, planes_rep, stride=16), :] = turn
        for t, first, size in tiles:
            zmodes[:, part, strip, first : first + size] = (
                spread[t, :, :size].reshape(planes_rep, 16, size).astype(jnp.bfloat16)
            )
        return carry

    def send_modes(p, carry):
        target = owner_of(p)
        for dh in range(row_count):
            target_row = lax.rem(row + dh, row_count)
            if dh:
                mode_copy(p, row, me, target_row, target).start()
            else:
                @pl.when(target != me)
                def _():
                    mode_copy(p, row, me, target_row, target).start()

                @pl.when(target == me)
                def _():
                    mode_keep(p).start()
        return carry

    def inside(p):
        return jnp.logical_and(p >= 0, p < planes)

    own_points = pl.ds(pl.multiple_of(me * point_block, point_block), point_block)

    def project_noise(p):
        noise_copy(p).wait()
        slot = lax.rem(p, 2)
        step_of = max(c for c in (512, 256, 128) if point_count % c == 0)
        columns = None
        for first in range(0, point_count, step_of):
            span = slice(first, first + step_of)
            field = noise[slot, :, :, span].reshape(2 * point_block, step_of)
            more = lax.dot_general(table_ref[:, span], field, NT, preferred_element_type=jnp.float32)
            columns = more if columns is None else columns + more
        turned = turned_ref[own_points]
        for part in range(2):
            column = columns[:, part * point_block : (part + 1) * point_block].astype(jnp.bfloat16)
            parts[p, part] = jnp.dot(column, turned, preferred_element_type=jnp.float32).astype(
                jnp.bfloat16
            )

        @pl.when(p + 2 < planes)
        def _():
            noise_copy(p + 2).start()

    def wait_modes(k):
        p = plane_of(k)
        for h in range(row_count):
            for j in range(count):
                mine = jnp.logical_and(row == h, me == j)

                @pl.when(mine)
                def _():
                    mode_keep(p).wait()

                @pl.when(jnp.logical_not(mine))
                def _():
                    mode_copy(p, h, j, row, me).wait_recv()

    def cubic_unit(u, carry):
        k = lax.div(u, units)
        at = lax.rem(u, units)

        @pl.when(at == 0)
        def _():
            wait_modes(k)

        span = pl.ds(pl.multiple_of(at * width, width), width)
        for part in range(2):
            line = None
            for h in range(row_count):
                more = jnp.dot(
                    modes[k, h, part], table_ref[h * row_block : (h + 1) * row_block, span],
                    preferred_element_type=jnp.float32,
                )
                line = more if line is None else line + more
            lines[:, part * width : (part + 1) * width] = line.astype(jnp.bfloat16)
        columns = None
        for first in range(0, point_count, chunk):
            wave = jnp.dot(
                turned_ref[first : first + chunk], lines[...], preferred_element_type=jnp.float32
            )
            wave_real, wave_imag = wave[:, :width], wave[:, width:]
            density = wave_real * wave_real + wave_imag * wave_imag
            drive = jnp.concatenate(
                [
                    (density * (wave_imag - DAMPING * wave_real)).astype(jnp.bfloat16),
                    (density * (-wave_real - DAMPING * wave_imag)).astype(jnp.bfloat16),
                ],
                1,
            )
            more = jnp.dot(
                table_ref[:, first : first + chunk], drive, preferred_element_type=jnp.float32
            )
            columns = more if columns is None else columns + more
        for part in range(2):
            more = jnp.dot(
                columns[:, part * width : (part + 1) * width].astype(jnp.bfloat16),
                turned_ref[span], preferred_element_type=jnp.float32,
            )

            @pl.when(at == 0)
            def _():
                total[part] = more

            @pl.when(at > 0)
            def _():
                total[part] += more

        @pl.when(at == units - 1)
        def _():
            cubic[k] = total[...].astype(jnp.bfloat16)

        return carry

    def add(p, j, slot):
        both = parts[p, :, rows(j)].astype(jnp.float32) + landed[p, slot].astype(jnp.float32)
        parts[p, :, rows(j)] = both.astype(jnp.bfloat16)

    rise_lag = jnp.where(me == 0, lag_end, lag_mid + me - 1)
    sink_lag = jnp.where(me == count - 1, lag_end, lag_mid + count - 2 - me)
    merge_lag = jnp.minimum(rise_lag, sink_lag)
    done_lag = jnp.maximum(rise_lag, sink_lag)

    def step(s, carry):
        @pl.when(s < planes)
        def _():
            project_noise(s)

        merging = s - merge_lag

        @pl.when(jnp.logical_and(inside(merging), owner_of(merging) == me))
        def _():
            both = parts[merging].astype(jnp.float32) + cubic[slot_of(merging)].astype(jnp.float32)
            parts[merging] = both.astype(jnp.bfloat16)

        rising = s - rise_lag
        sinking = s - sink_lag

        @pl.when(jnp.logical_and(inside(rising), me == 0))
        def _():
            for j in range(count - 1, 0, -1):
                sum_copy(rising, j, 0, j).start()

        @pl.when(jnp.logical_and(inside(sinking), me == count - 1))
        def _():
            for j in range(count - 1):
                sum_copy(sinking, j, 1, count if j == count - 2 else j).start()

        @pl.when(s == modes_step)
        def _():
            lax.fori_loop(0, 2 * strips, contract_strip, 0)
            lax.fori_loop(0, planes, send_modes, 0)

        unit = (s - cubic_step) * rate
        lax.fori_loop(
            jnp.clip(unit, 0, per * units), jnp.clip(unit + rate, 0, per * units), cubic_unit, 0
        )

        for far in range(count - 2, 0, -1):
            @pl.when(jnp.logical_and(jnp.logical_and(inside(rising), has_down), me + far <= count - 1))
            def _():
                j = me + far
                sum_copy(rising, j, 0, j).wait_recv()
                add(rising, j, j)
                sum_copy(rising, j, 0, j).start()

        for far in range(count - 2, 0, -1):
            @pl.when(jnp.logical_and(jnp.logical_and(inside(sinking), has_up), me - far >= 0))
            def _():
                j = me - far
                sum_copy(sinking, j, 1, j).wait_recv()
                add(sinking, j, j)
                sum_copy(sinking, j, 1, count if far == 1 else j).start()

        done = s - done_lag

        @pl.when(inside(done))
        def _():
            @pl.when(has_down)
            def _():
                sum_copy(done, me, 0, me).wait_recv()
                add(done, me, me)

            @pl.when(has_up)
            def _():
                sum_copy(done, me, 1, count).wait_recv()
                add(done, me, count)

            for part in range(2):
                whole = parts[done, part, rows(me)]
                for h in range(row_count):
                    halves[done, h, part] = whole[:, h * row_block : (h + 1) * row_block]
            for at in range(len(spots) - 1, -1, -1):
                first_copy(done, at, False).start()
            if pair == 2:
                second_copy(done, 0, False).start()

        passing = done - 1

        @pl.when(inside(passing))
        def _():
            for at in range(1, len(spots)):
                first_copy(passing, at, True).wait_recv()
                if pair == 2:
                    second_copy(passing, at, False).start()

        return carry

    lax.fori_loop(0, planes + lag_mid + count - 1, step, 0)

    def finish(p, carry):
        for j in range(count):
            @pl.when(j > me)
            def _():
                sum_copy(p, j, 0, j).wait_send()

            @pl.when(j < me)
            def _():
                sum_copy(p, j, 1, j).wait_send()

        target = owner_of(p)
        for dh in range(row_count):
            target_row = lax.rem(row + dh, row_count)
            if dh:
                mode_copy(p, row, me, target_row, target).wait_send()
            else:
                @pl.when(target != me)
                def _():
                    mode_copy(p, row, me, target_row, target).wait_send()

        first_copy(p, 0, False).wait()
        for at in range(len(spots)):
            if at:
                first_copy(p, at, False).wait_send()
            if pair == 2:
                second_copy(p, at, False).wait_send()
                second_copy(p, at, True).wait_recv()
        return carry

    lax.fori_loop(0, planes, finish, 0)


def slab_planes(coefficients, noise_field, mode_table, turned, slab_own):
    count = lax.axis_size("my")
    mode_count = mode_table.shape[0]
    row_count = lax.axis_size("mx")
    rep_count = lax.axis_size("rep")
    _, row_block, block, depth = coefficients.shape
    planes = noise_field.shape[0]
    planes_rep = planes * row_count
    per = planes // count
    spots = row_count * (rep_count // (2 if rep_count % 2 == 0 else 1))
    point_block, point_count = noise_field.shape[2:]
    width = max(c for c in (256, 128) if point_count % c == 0)
    lanes = slab_own.shape[1]
    vmem = pl.BlockSpec(memory_space=pltpu.VMEM)
    hbm = pl.BlockSpec(memory_space=pl.ANY)
    dma = pltpu.SemaphoreType.DMA
    flops = 12 * planes * mode_count * point_block * (point_count + mode_count)
    return pl.pallas_call(
        slab_kernel,
        out_shape=jax.ShapeDtypeStruct((planes_rep * rep_count, 2, block, row_block), jnp.bfloat16),
        in_specs=[hbm, hbm, vmem, vmem, vmem],
        out_specs=hbm,
        scratch_shapes=[
            pltpu.VMEM((2, row_block, 16, depth), jnp.bfloat16),
            pltpu.VMEM((row_block * 16, lanes), jnp.float32),
            pltpu.VMEM((pl.cdiv(row_block, 128), planes_rep * 16, 128), jnp.float32),
            pltpu.VMEM((planes_rep, 2, block, row_block), jnp.bfloat16),
            pltpu.VMEM((per, row_count, 2, mode_count, row_block), jnp.bfloat16),
            pltpu.VMEM((mode_count, 2 * width), jnp.bfloat16),
            pltpu.VMEM((2, mode_count, mode_count), jnp.float32),
            pltpu.VMEM((per, 2, mode_count, mode_count), jnp.bfloat16),
            pltpu.VMEM((planes, 2, mode_count, mode_count), jnp.bfloat16),
            pltpu.VMEM((planes, count + 1, 2, block, mode_count), jnp.bfloat16),
            pltpu.VMEM((2, 2, point_block, point_count), jnp.bfloat16),
            pltpu.VMEM((planes, row_count, 2, block, row_block), jnp.bfloat16),
            dma((2,)),
            dma((2,)),
            dma((per, row_count, count)),
            dma((planes, row_count)),
            dma((planes, count + 1)),
            dma((planes, 2, count)),
            dma((planes, spots)),
            dma((planes, spots)),
            dma((planes, spots)),
            dma((planes, spots)),
        ],
        compiler_params=pltpu.CompilerParams(
            collective_id=0, has_side_effects=True, vmem_limit_bytes=60 * 1024 * 1024
        ),
        cost_estimate=pl.CostEstimate(
            flops=flops, bytes_accessed=noise_field.size * 2, transcendentals=0
        ),
    )(coefficients, noise_field, mode_table, turned, slab_own)


def body(coefficients, noise_field, mode_table):
    rep_index = lax.axis_index("rep")
    rep_count = lax.axis_size("rep")
    row_count = lax.axis_size("mx")
    col_count = lax.axis_size("my")
    planes_dev = noise_field.shape[0]
    planes_rep = planes_dev * row_count
    planes_all = planes_rep * rep_count
    mode_count = mode_table.shape[0]
    point_count = mode_table.shape[1]
    slab_first = point_count // 2 - planes_all // 2
    row_block = mode_count // row_count
    col_block = mode_count // col_count
    point_block = point_count // col_count
    own_block = mode_count // rep_count
    if (
        col_block % 16 or row_block % 16 or point_block % 128 or mode_count % 128
        or col_count < 2 or col_count % 2 or planes_dev % col_count or planes_rep > 128 or planes_rep % 8
    ):
        return plain_body(coefficients, noise_field, mode_table)
    slab_own = lax.dynamic_slice_in_dim(
        mode_table, slab_first + rep_index * planes_rep, planes_rep, 1
    )
    slab_own = jnp.pad(slab_own, ((0, 0), (0, 128 - planes_rep)))
    plane_grid = slab_planes(coefficients, noise_field, mode_table, mode_table.T, slab_own)
    slab_back = lax.dynamic_slice_in_dim(mode_table, rep_index * own_block, own_block, 0)[
        :, slab_first : slab_first + planes_all
    ]
    summed = jnp.einsum("zpba,nz->pabn", plane_grid, slab_back, preferred_element_type=jnp.float32)
    return summed.astype(jnp.bfloat16)


def solution(mesh):
    in_specs = (P(None, "mx", "my", None), P(("rep", "mx"), None, "my", None), P())
    out_specs = P(None, "mx", "my", "rep")
    return jax.shard_map(body, mesh=mesh, in_specs=in_specs, out_specs=out_specs, check_vma=False)
```

```python
import jax
import jax.numpy as jnp
from jax import lax
from jax.experimental import pallas as pl
from jax.experimental.pallas import tpu as pltpu
from jax.sharding import PartitionSpec as P

DAMPING = 0.25
MESH = pl.DeviceIdType.MESH
NT = (((1,), (1,)), ((), ()))


def plain_body(coefficients, noise_field, mode_table):
    rep_index = lax.axis_index("rep")
    col_index = lax.axis_index("my")
    rep_count = lax.axis_size("rep")
    row_count = lax.axis_size("mx")
    col_count = lax.axis_size("my")
    planes_dev = noise_field.shape[0]
    planes_rep = planes_dev * row_count
    planes_all = planes_rep * rep_count
    mode_count = mode_table.shape[0]
    point_count = mode_table.shape[1]
    slab_first = point_count // 2 - planes_all // 2
    row_block = mode_count // row_count
    col_block = mode_count // col_count
    point_block = point_count // col_count
    own_block = mode_count // rep_count
    slab_own = lax.dynamic_slice_in_dim(
        mode_table, slab_first + rep_index * planes_rep, planes_rep, 1
    )
    zmodes = jnp.einsum(
        "pabk,kz->zpba", coefficients, slab_own, preferred_element_type=jnp.float32
    ).astype(jnp.bfloat16)
    zmodes = zmodes.reshape(planes_rep, 2, col_block * row_block)
    spread = lax.all_to_all(zmodes, "mx", split_axis=0, concat_axis=2, tiled=True)
    grouped = spread.reshape(planes_dev, 2, row_count, col_block, row_block)
    tiled_table = mode_table.reshape(row_count, row_block, point_count)
    own_points = lax.dynamic_slice_in_dim(tiled_table, col_index * point_block, point_block, 2)
    block_part = jnp.einsum(
        "zpsal,slx->zpax",
        lax.all_gather(grouped, "my", axis=3, tiled=True),
        own_points,
        preferred_element_type=jnp.float32,
    ).astype(jnp.bfloat16)
    wave_field = jnp.einsum(
        "zpax,ay->zpxy", block_part, mode_table, preferred_element_type=jnp.float32
    )
    wave_real = wave_field[:, 0]
    wave_imag = wave_field[:, 1]
    density = wave_real * wave_real + wave_imag * wave_imag
    noise_wide = noise_field.astype(jnp.float32)
    drive_term = jnp.stack(
        [
            density * (wave_imag - DAMPING * wave_real) + noise_wide[:, 0],
            density * (-wave_real - DAMPING * wave_imag) + noise_wide[:, 1],
        ],
        1,
    ).astype(jnp.bfloat16)
    proj_columns = jnp.einsum(
        "zpxy,ny->zpnx", drive_term, mode_table, preferred_element_type=jnp.float32
    ).astype(jnp.bfloat16)
    block_part = lax.all_to_all(proj_columns, "my", split_axis=2, concat_axis=3, tiled=True)
    folded = jnp.einsum(
        "zpax,slx->zpsal", block_part, tiled_table, preferred_element_type=jnp.float32
    ).astype(jnp.bfloat16)
    proj_rows = folded.reshape(
        block_part.shape[0], block_part.shape[1], row_count * col_block * row_block
    )
    gathered_rows = lax.all_to_all(proj_rows, "mx", split_axis=2, concat_axis=0, tiled=True)
    slab_back = lax.dynamic_slice_in_dim(mode_table, rep_index * own_block, own_block, 0)[
        :, slab_first : slab_first + planes_all
    ]
    portion = lax.all_gather(gathered_rows, "rep", axis=0, tiled=True)
    plane_grid = portion.reshape(portion.shape[0], 2, col_block, row_block)
    summed = jnp.einsum("zpba,nz->pabn", plane_grid, slab_back, preferred_element_type=jnp.float32)
    return summed.astype(jnp.bfloat16)

def slab_owners(planes, count):
    half = count // 2
    inner = max(1, planes // count // 2)
    shared = 2 * inner * (half - 1)
    return half, inner, shared, (planes - shared) // 2


def slab_schedule(planes, count, units, rate, first_step):
    half, inner, shared, outer = slab_owners(planes, count)

    def needed(me):
        group = me - half if me >= half else half - 1 - me
        owned = inner if group < half - 1 else outer
        first = group * 2 * inner + (1 if me >= half else 0)
        ready = [first_step + ((k + 1) * units - 1) // rate for k in range(owned)]
        return max(ready[k] + 1 - first - 2 * k for k in range(owned))

    lag_end = max(0, needed(0), needed(count - 1))
    lag_mid = max([lag_end + 1] + [needed(me) for me in range(1, count - 1)])
    return lag_end, lag_mid


def slab_kernel(coef_ref, noise_ref, table_ref, turned_ref, slab_ref, out_ref, coef, wide, spread, zmodes,
                modes, split, lines, total, cubic, parts, landed, noise, halves, coef_sem, noise_sem, mode_recv,
                mode_send, sum_recv, sum_send, first_recv, first_send, second_recv, second_send):
    count = lax.axis_size("my")
    me = lax.axis_index("my")
    row_count = lax.axis_size("mx")
    row = lax.axis_index("mx")
    rep_count = lax.axis_size("rep")
    rep = lax.axis_index("rep")
    planes = noise_ref.shape[0]
    planes_rep = planes * row_count
    row_block = coef_ref.shape[1]
    block = coef_ref.shape[2]
    pair = 2 if rep_count % 2 == 0 else 1
    groups = rep_count // pair
    group = lax.div(rep, pair)
    side = lax.rem(rep, pair)
    spots = [(dg, dh) for dg in range(groups) for dh in range(row_count)]
    offsets = [(dr, dh) for dr in range(rep_count) for dh in range(row_count)]
    full = row_block // 128
    rest = row_block % 128
    pieces = zmodes.shape[1]
    mode_count, point_count = table_ref.shape
    point_block = noise_ref.shape[2]
    width = lines.shape[1] // 2
    units = point_count // width
    chunk = 256 if point_count % 256 == 0 else 128
    rate = max(1, units // 2)
    modes_step, cubic_step = 2, 4
    half, inner, shared, outer = slab_owners(planes, count)
    lag_end, lag_mid = slab_schedule(planes, count, units, rate, cubic_step)
    tail = max(0, planes - 4)
    up = {"my": me + 1}
    down = {"my": me - 1}
    has_up = me < count - 1
    has_down = me > 0

    barrier = pltpu.get_barrier_semaphore()
    line_peers = [(dh, dm) for dh in range(row_count) for dm in range(count)][1:]
    rep_peers = [(dr, dh) for dr, dh in offsets if dr > 0]
    for dh, dm in line_peers:
        pl.semaphore_signal(
            barrier, inc=1,
            device_id={"mx": lax.rem(row + dh, row_count), "my": lax.rem(me + dm, count)},
            device_id_type=MESH,
        )
    for dr, dh in rep_peers:
        pl.semaphore_signal(
            barrier, inc=1,
            device_id={"rep": lax.rem(rep + dr, rep_count), "mx": lax.rem(row + dh, row_count)},
            device_id_type=MESH,
        )

    def rows(j):
        return pl.ds(pl.multiple_of(j * block, block), block)

    def group_of(p):
        return jnp.minimum(lax.div(p, 2 * inner), half - 1)

    def owner_of(p):
        return jnp.where(lax.rem(p, 2) == 1, half + group_of(p), half - 1 - group_of(p))

    def slot_of(p):
        return lax.div(p - group_of(p) * (2 * inner), 2)

    own_group = jnp.where(me >= half, me - half, half - 1 - me)
    owned = jnp.where(own_group < half - 1, inner, outer)

    def plane_of(k):
        return own_group * (2 * inner) + 2 * k + (me >= half).astype(jnp.int32)

    def mode_copy(p, h, j, target_row, target):
        return pltpu.make_async_remote_copy(
            src_ref=zmodes.at[target_row * planes + p],
            dst_ref=modes.at[slot_of(p), h, :, rows(j)],
            send_sem=mode_send.at[p, target_row],
            recv_sem=mode_recv.at[slot_of(p), h, j],
            device_id={"mx": target_row, "my": target},
            device_id_type=MESH,
        )

    def mode_keep(p):
        return pltpu.make_async_copy(
            zmodes.at[row * planes + p], modes.at[slot_of(p), row, :, rows(me)],
            mode_recv.at[slot_of(p), row, me],
        )

    def plane_at(from_group, from_side, from_row, p):
        return ((from_group * pair + from_side) * row_count + from_row) * planes + p

    def first_copy(p, at, received):
        dg, dh = spots[at]
        target_row = lax.rem(row + dh, row_count)
        if at == 0:
            return pltpu.make_async_copy(
                halves.at[p, row], out_ref.at[plane_at(group, side, row, p)], first_send.at[p, 0]
            )
        if received:
            plane = plane_at(
                lax.rem(group + groups - dg, groups), side, lax.rem(row + row_count - dh, row_count), p
            )
        else:
            plane = plane_at(group, side, row, p)
        return pltpu.make_async_remote_copy(
            src_ref=halves.at[p, target_row],
            dst_ref=out_ref.at[plane],
            send_sem=first_send.at[p, at],
            recv_sem=first_recv.at[p, at],
            device_id={"rep": lax.rem(group + dg, groups) * pair + side, "mx": target_row},
            device_id_type=MESH,
        )

    def second_copy(p, at, received):
        dg, dh = spots[at]
        plane = plane_at(
            lax.rem(group + groups - dg, groups), 1 - side if received else side,
            lax.rem(row + row_count - dh, row_count), p,
        )
        return pltpu.make_async_remote_copy(
            src_ref=halves.at[p, row] if at == 0 else out_ref.at[plane],
            dst_ref=out_ref.at[plane],
            send_sem=second_send.at[p, at],
            recv_sem=second_recv.at[p, at],
            device_id={"rep": group * pair + 1 - side},
            device_id_type=MESH,
        )

    def noise_copy(p):
        slot = lax.rem(p, 2)
        return pltpu.make_async_copy(noise_ref.at[p], noise.at[slot], noise_sem.at[slot])

    def sum_copy(p, j, way, slot):
        return pltpu.make_async_remote_copy(
            src_ref=parts.at[p, :, rows(j)],
            dst_ref=landed.at[p, slot],
            send_sem=sum_send.at[p, way, j],
            recv_sem=sum_recv.at[p, slot],
            device_id=down if way else up,
            device_id_type=MESH,
        )

    strips = block // 16

    def coef_copy(i, part):
        strip = pl.ds(pl.multiple_of(i * 16, 16), 16)
        return pltpu.make_async_copy(coef_ref.at[part, :, strip], coef.at[part], coef_sem.at[part])

    noise_copy(0).start()
    if planes > 1:
        noise_copy(1).start()
    coef_copy(0, 0).start()
    coef_copy(0, 1).start()

    pl.semaphore_wait(barrier, len(line_peers) + len(rep_peers))

    def split_table():
        split[...] = jnp.zeros_like(split)
        for h in range(row_count):
            for part in range(2):
                for t in range(full + (1 if rest else 0)):
                    size = min(128, row_block - t * 128)
                    source = h * row_block + t * 128
                    place = (h * (full + (1 if rest else 0)) + t) * 128 + (part * rest if size < 128 else 0)
                    split[part, place : place + size] = table_ref[source : source + size]

    def contract_strip(i, carry):
        strip = pl.ds(pl.multiple_of(i * 16, 16), 16)
        for part in range(2):
            coef_copy(i, part).wait()
            wide[part] = jnp.dot(
                coef[part].reshape(row_block * 16, coef.shape[3]), slab_ref[...],
                preferred_element_type=jnp.float32,
            )

            @pl.when(i + 1 < strips)
            def _():
                coef_copy(i + 1, part).start()

        for b in range(16):
            for part in range(2):
                for t in range(full):
                    turn = wide[part, pl.ds(t * 2048 + b, 128, stride=16), :].T[:planes_rep]
                    spread[part * full + t, pl.ds(b, planes_rep, stride=16), :] = turn
            if rest:
                both = [wide[part, pl.ds(full * 2048 + b, rest, stride=16), :] for part in range(2)]
                spread[2 * full, pl.ds(b, planes_rep, stride=16), :] = jnp.concatenate(both, 0).T[:planes_rep]
        for t in range(pieces):
            zmodes[:, t, strip, :] = spread[t].reshape(planes_rep, 16, 128).astype(jnp.bfloat16)
        return carry

    def send_modes(p, carry):
        target = owner_of(p)
        for dh in range(row_count):
            target_row = lax.rem(row + dh, row_count)
            if dh:
                mode_copy(p, row, me, target_row, target).start()
            else:
                @pl.when(target != me)
                def _():
                    mode_copy(p, row, me, target_row, target).start()

                @pl.when(target == me)
                def _():
                    mode_keep(p).start()
        return carry

    def inside(p):
        return jnp.logical_and(p >= 0, p < planes)

    def span_of(i):
        low = jnp.where(i == planes - 1, tail, i)
        valid = jnp.logical_and(i >= 0, jnp.logical_or(i < tail, i == planes - 1))
        return low, jnp.where(valid, i + 1, low)

    own_points = pl.ds(pl.multiple_of(me * point_block, point_block), point_block)

    def project_noise(p):
        noise_copy(p).wait()
        slot = lax.rem(p, 2)
        step_of = max(c for c in (512, 256, 128) if point_count % c == 0)
        columns = None
        for first in range(0, point_count, step_of):
            span = slice(first, first + step_of)
            field = noise[slot, :, :, span].reshape(2 * point_block, step_of)
            more = lax.dot_general(table_ref[:, span], field, NT, preferred_element_type=jnp.float32)
            columns = more if columns is None else columns + more
        turned = turned_ref[own_points]
        for part in range(2):
            column = columns[:, part * point_block : (part + 1) * point_block].astype(jnp.bfloat16)
            parts[p, part] = jnp.dot(column, turned, preferred_element_type=jnp.float32).astype(
                jnp.bfloat16
            )

        @pl.when(p + 2 < planes)
        def _():
            noise_copy(p + 2).start()

    def wait_modes(k):
        p = plane_of(k)
        for h in range(row_count):
            for j in range(count):
                mine = jnp.logical_and(row == h, me == j)

                @pl.when(mine)
                def _():
                    mode_keep(p).wait()

                @pl.when(jnp.logical_not(mine))
                def _():
                    mode_copy(p, h, j, row, me).wait_recv()

    def cubic_unit(u, carry):
        k = lax.div(u, units)
        at = lax.rem(u, units)

        @pl.when(at == 0)
        def _():
            wait_modes(k)

        span = pl.ds(pl.multiple_of(at * width, width), width)
        for part in range(2):
            field = []
            for h in range(row_count):
                field += [modes[k, h, part * full + t] for t in range(full)]
                if rest:
                    field.append(modes[k, h, 2 * full])
            line = jnp.dot(
                jnp.concatenate(field, 1), split[part, :, span], preferred_element_type=jnp.float32
            )
            lines[:, part * width : (part + 1) * width] = line.astype(jnp.bfloat16)
        columns = None
        for first in range(0, point_count, chunk):
            wave = jnp.dot(
                turned_ref[first : first + chunk], lines[...], preferred_element_type=jnp.float32
            )
            wave_real, wave_imag = wave[:, :width], wave[:, width:]
            density = wave_real * wave_real + wave_imag * wave_imag
            drive = jnp.concatenate(
                [
                    (density * (wave_imag - DAMPING * wave_real)).astype(jnp.bfloat16),
                    (density * (-wave_real - DAMPING * wave_imag)).astype(jnp.bfloat16),
                ],
                1,
            )
            more = jnp.dot(
                table_ref[:, first : first + chunk], drive, preferred_element_type=jnp.float32
            )
            columns = more if columns is None else columns + more
        for part in range(2):
            more = jnp.dot(
                columns[:, part * width : (part + 1) * width].astype(jnp.bfloat16),
                turned_ref[span], preferred_element_type=jnp.float32,
            )

            @pl.when(at == 0)
            def _():
                total[part] = more

            @pl.when(at > 0)
            def _():
                total[part] += more

        @pl.when(at == units - 1)
        def _():
            cubic[k] = total[...].astype(jnp.bfloat16)

        return carry

    def add(p, j, slot):
        both = parts[p, :, rows(j)].astype(jnp.float32) + landed[p, slot].astype(jnp.float32)
        parts[p, :, rows(j)] = both.astype(jnp.bfloat16)

    rise_lag = jnp.where(me == 0, lag_end, lag_mid + me - 1)
    sink_lag = jnp.where(me == count - 1, lag_end, lag_mid + count - 2 - me)
    merge_lag = jnp.minimum(rise_lag, sink_lag)
    done_lag = jnp.maximum(rise_lag, sink_lag)

    def step(s, carry):
        @pl.when(s < planes)
        def _():
            project_noise(s)

        sent = jnp.where(s < shared, s, s - lag_end)
        at_end = jnp.logical_or(me == 0, me == count - 1)
        merging = jnp.where(at_end, sent, s - merge_lag)

        @pl.when(jnp.logical_and(inside(merging), owner_of(merging) == me))
        def _():
            both = parts[merging].astype(jnp.float32) + cubic[slot_of(merging)].astype(jnp.float32)
            parts[merging] = both.astype(jnp.bfloat16)

        low, high = span_of(sent)
        high = jnp.where(jnp.logical_or(s < shared, sent >= shared), high, low)

        @pl.when(me == 0)
        def _():
            for j in range(count - 1, 0, -1):
                def emit(p, carry):
                    sum_copy(p, j, 0, j).start()
                    return carry

                lax.fori_loop(low, high, emit, 0)

        @pl.when(me == count - 1)
        def _():
            for j in range(count - 1):
                def emit(p, carry):
                    sum_copy(p, j, 1, count if j == count - 2 else j).start()
                    return carry

                lax.fori_loop(low, high, emit, 0)

        @pl.when(s == modes_step)
        def _():
            lax.fori_loop(0, strips, contract_strip, 0)
            lax.fori_loop(0, planes, send_modes, 0)

        unit = (s - cubic_step) * rate
        lax.fori_loop(
            jnp.clip(unit, 0, owned * units), jnp.clip(unit + rate, 0, owned * units), cubic_unit, 0
        )

        low, high = span_of(s - rise_lag)
        for far in range(count - 2, 0, -1):
            @pl.when(jnp.logical_and(has_down, me + far <= count - 1))
            def _():
                j = me + far

                def relay(p, carry):
                    sum_copy(p, j, 0, j).wait_recv()
                    add(p, j, j)
                    sum_copy(p, j, 0, j).start()
                    return carry

                lax.fori_loop(low, high, relay, 0)

        low, high = span_of(s - sink_lag)
        for far in range(count - 2, 0, -1):
            @pl.when(jnp.logical_and(has_up, me - far >= 0))
            def _():
                j = me - far

                def relay(p, carry):
                    sum_copy(p, j, 1, j).wait_recv()
                    add(p, j, j)
                    sum_copy(p, j, 1, count if far == 1 else j).start()
                    return carry

                lax.fori_loop(low, high, relay, 0)

        def finish_plane(p, carry):
            @pl.when(has_down)
            def _():
                sum_copy(p, me, 0, me).wait_recv()
                add(p, me, me)

            @pl.when(has_up)
            def _():
                sum_copy(p, me, 1, count).wait_recv()
                add(p, me, count)

            whole = [parts[p, part, rows(me)] for part in range(2)]
            for h in range(row_count):
                for part in range(2):
                    for t in range(full):
                        place = h * row_block + t * 128
                        halves[p, h, part * full + t] = whole[part][:, place : place + 128]
                if rest:
                    place = h * row_block + full * 128
                    halves[p, h, 2 * full] = jnp.concatenate(
                        [whole[part][:, place : place + rest] for part in range(2)], 1
                    )
            for at in range(len(spots) - 1, -1, -1):
                first_copy(p, at, False).start()
            if pair == 2:
                second_copy(p, 0, False).start()
            return carry

        low, high = span_of(s - done_lag)
        lax.fori_loop(low, high, finish_plane, 0)

        def pass_on(p, carry):
            for at in range(1, len(spots)):
                first_copy(p, at, True).wait_recv()
                if pair == 2:
                    second_copy(p, at, False).start()
            return carry

        low, high = span_of(s - done_lag - 1)
        lax.fori_loop(low, high, pass_on, 0)
        return carry

    split_table()
    lax.fori_loop(0, planes + lag_mid + count - 1, step, 0)

    def finish(p, carry):
        for j in range(count):
            @pl.when(j > me)
            def _():
                sum_copy(p, j, 0, j).wait_send()

            @pl.when(j < me)
            def _():
                sum_copy(p, j, 1, j).wait_send()

        target = owner_of(p)
        for dh in range(row_count):
            target_row = lax.rem(row + dh, row_count)
            if dh:
                mode_copy(p, row, me, target_row, target).wait_send()
            else:
                @pl.when(target != me)
                def _():
                    mode_copy(p, row, me, target_row, target).wait_send()

        first_copy(p, 0, False).wait()
        for at in range(len(spots)):
            if at:
                first_copy(p, at, False).wait_send()
            if pair == 2:
                second_copy(p, at, False).wait_send()
                second_copy(p, at, True).wait_recv()
        return carry

    lax.fori_loop(0, planes, finish, 0)


def slab_planes(coefficients, noise_field, mode_table, turned, slab_own):
    count = lax.axis_size("my")
    mode_count = mode_table.shape[0]
    row_count = lax.axis_size("mx")
    rep_count = lax.axis_size("rep")
    _, row_block, block, depth = coefficients.shape
    planes = noise_field.shape[0]
    planes_rep = planes * row_count
    outer = slab_owners(planes, count)[3]
    pieces = 2 * row_block // 128
    places = row_count * pl.cdiv(row_block, 128) * 128
    spots = row_count * (rep_count // (2 if rep_count % 2 == 0 else 1))
    point_block, point_count = noise_field.shape[2:]
    width = max(c for c in (256, 128) if point_count % c == 0)
    lanes = slab_own.shape[1]
    vmem = pl.BlockSpec(memory_space=pltpu.VMEM)
    hbm = pl.BlockSpec(memory_space=pl.ANY)
    dma = pltpu.SemaphoreType.DMA
    flops = 12 * planes * mode_count * point_block * (point_count + mode_count)
    return pl.pallas_call(
        slab_kernel,
        out_shape=jax.ShapeDtypeStruct((planes_rep * rep_count, pieces, block, 128), jnp.bfloat16),
        in_specs=[hbm, hbm, vmem, vmem, vmem],
        out_specs=hbm,
        scratch_shapes=[
            pltpu.VMEM((2, row_block, 16, depth), jnp.bfloat16),
            pltpu.VMEM((2, row_block * 16, lanes), jnp.float32),
            pltpu.VMEM((pieces, planes_rep * 16, 128), jnp.float32),
            pltpu.VMEM((planes_rep, pieces, block, 128), jnp.bfloat16),
            pltpu.VMEM((outer, row_count, pieces, mode_count, 128), jnp.bfloat16),
            pltpu.VMEM((2, places, point_count), jnp.bfloat16),
            pltpu.VMEM((mode_count, 2 * width), jnp.bfloat16),
            pltpu.VMEM((2, mode_count, mode_count), jnp.float32),
            pltpu.VMEM((outer, 2, mode_count, mode_count), jnp.bfloat16),
            pltpu.VMEM((planes, 2, mode_count, mode_count), jnp.bfloat16),
            pltpu.VMEM((planes, count + 1, 2, block, mode_count), jnp.bfloat16),
            pltpu.VMEM((2, 2, point_block, point_count), jnp.bfloat16),
            pltpu.VMEM((planes, row_count, pieces, block, 128), jnp.bfloat16),
            dma((2,)),
            dma((2,)),
            dma((outer, row_count, count)),
            dma((planes, row_count)),
            dma((planes, count + 1)),
            dma((planes, 2, count)),
            dma((planes, spots)),
            dma((planes, spots)),
            dma((planes, spots)),
            dma((planes, spots)),
        ],
        compiler_params=pltpu.CompilerParams(
            collective_id=0, has_side_effects=True, vmem_limit_bytes=60 * 1024 * 1024
        ),
        cost_estimate=pl.CostEstimate(
            flops=flops, bytes_accessed=noise_field.size * 2, transcendentals=0
        ),
    )(coefficients, noise_field, mode_table, turned, slab_own)


def body(coefficients, noise_field, mode_table):
    rep_index = lax.axis_index("rep")
    rep_count = lax.axis_size("rep")
    row_count = lax.axis_size("mx")
    col_count = lax.axis_size("my")
    planes_dev = noise_field.shape[0]
    planes_rep = planes_dev * row_count
    planes_all = planes_rep * rep_count
    mode_count = mode_table.shape[0]
    point_count = mode_table.shape[1]
    slab_first = point_count // 2 - planes_all // 2
    row_block = mode_count // row_count
    col_block = mode_count // col_count
    point_block = point_count // col_count
    own_block = mode_count // rep_count
    if (
        col_block % 16 or row_block % 16 or point_block % 128 or mode_count % 128
        or row_block % 64 or col_count < 2 or col_count % 2 or planes_dev % (2 * col_count)
        or planes_rep > 128 or planes_rep % 8
    ):
        return plain_body(coefficients, noise_field, mode_table)
    slab_own = lax.dynamic_slice_in_dim(
        mode_table, slab_first + rep_index * planes_rep, planes_rep, 1
    )
    slab_own = jnp.pad(slab_own, ((0, 0), (0, 128 - planes_rep)))
    plane_grid = slab_planes(coefficients, noise_field, mode_table, mode_table.T, slab_own)
    slab_back = lax.dynamic_slice_in_dim(mode_table, rep_index * own_block, own_block, 0)[
        :, slab_first : slab_first + planes_all
    ]
    summed = jnp.einsum("ztbl,nz->tlbn", plane_grid, slab_back, preferred_element_type=jnp.float32)
    summed = summed.astype(jnp.bfloat16)
    full, rest = row_block // 128, row_block % 128
    halves = []
    for part in range(2):
        lines = [summed[part * full + t] for t in range(full)]
        if rest:
            lines.append(summed[2 * full, part * rest : (part + 1) * rest])
        halves.append(jnp.concatenate(lines, 0))
    return jnp.stack(halves)


def solution(mesh):
    in_specs = (P(None, "mx", "my", None), P(("rep", "mx"), None, "my", None), P())
    out_specs = P(None, "mx", "my", "rep")
    return jax.shard_map(body, mesh=mesh, in_specs=in_specs, out_specs=out_specs, check_vma=False)
```

```python
import jax
import jax.numpy as jnp
from jax import lax
from jax.experimental import pallas as pl
from jax.experimental.pallas import tpu as pltpu
from jax.sharding import PartitionSpec as P

DAMPING = 0.25
MESH = pl.DeviceIdType.MESH
NT = (((1,), (1,)), ((), ()))


def plain_body(coefficients, noise_field, mode_table):
    rep_index = lax.axis_index("rep")
    col_index = lax.axis_index("my")
    rep_count = lax.axis_size("rep")
    row_count = lax.axis_size("mx")
    col_count = lax.axis_size("my")
    planes_dev = noise_field.shape[0]
    planes_rep = planes_dev * row_count
    planes_all = planes_rep * rep_count
    mode_count = mode_table.shape[0]
    point_count = mode_table.shape[1]
    slab_first = point_count // 2 - planes_all // 2
    row_block = mode_count // row_count
    col_block = mode_count // col_count
    point_block = point_count // col_count
    own_block = mode_count // rep_count
    slab_own = lax.dynamic_slice_in_dim(
        mode_table, slab_first + rep_index * planes_rep, planes_rep, 1
    )
    zmodes = jnp.einsum(
        "pabk,kz->zpba", coefficients, slab_own, preferred_element_type=jnp.float32
    ).astype(jnp.bfloat16)
    zmodes = zmodes.reshape(planes_rep, 2, col_block * row_block)
    spread = lax.all_to_all(zmodes, "mx", split_axis=0, concat_axis=2, tiled=True)
    grouped = spread.reshape(planes_dev, 2, row_count, col_block, row_block)
    tiled_table = mode_table.reshape(row_count, row_block, point_count)
    own_points = lax.dynamic_slice_in_dim(tiled_table, col_index * point_block, point_block, 2)
    block_part = jnp.einsum(
        "zpsal,slx->zpax",
        lax.all_gather(grouped, "my", axis=3, tiled=True),
        own_points,
        preferred_element_type=jnp.float32,
    ).astype(jnp.bfloat16)
    wave_field = jnp.einsum(
        "zpax,ay->zpxy", block_part, mode_table, preferred_element_type=jnp.float32
    )
    wave_real = wave_field[:, 0]
    wave_imag = wave_field[:, 1]
    density = wave_real * wave_real + wave_imag * wave_imag
    noise_wide = noise_field.astype(jnp.float32)
    drive_term = jnp.stack(
        [
            density * (wave_imag - DAMPING * wave_real) + noise_wide[:, 0],
            density * (-wave_real - DAMPING * wave_imag) + noise_wide[:, 1],
        ],
        1,
    ).astype(jnp.bfloat16)
    proj_columns = jnp.einsum(
        "zpxy,ny->zpnx", drive_term, mode_table, preferred_element_type=jnp.float32
    ).astype(jnp.bfloat16)
    block_part = lax.all_to_all(proj_columns, "my", split_axis=2, concat_axis=3, tiled=True)
    folded = jnp.einsum(
        "zpax,slx->zpsal", block_part, tiled_table, preferred_element_type=jnp.float32
    ).astype(jnp.bfloat16)
    proj_rows = folded.reshape(
        block_part.shape[0], block_part.shape[1], row_count * col_block * row_block
    )
    gathered_rows = lax.all_to_all(proj_rows, "mx", split_axis=2, concat_axis=0, tiled=True)
    slab_back = lax.dynamic_slice_in_dim(mode_table, rep_index * own_block, own_block, 0)[
        :, slab_first : slab_first + planes_all
    ]
    portion = lax.all_gather(gathered_rows, "rep", axis=0, tiled=True)
    plane_grid = portion.reshape(portion.shape[0], 2, col_block, row_block)
    summed = jnp.einsum("zpba,nz->pabn", plane_grid, slab_back, preferred_element_type=jnp.float32)
    return summed.astype(jnp.bfloat16)

def slab_owners(planes, count):
    half = count // 2
    inner = max(1, 3 * planes // (4 * count))
    shared = 2 * inner * (half - 1)
    return half, inner, shared, (planes - shared) // 2


def slab_schedule(planes, count, units, rate, first_step):
    half, inner, shared, outer = slab_owners(planes, count)

    def needed(me):
        group = me - half if me >= half else half - 1 - me
        owned = inner if group < half - 1 else outer
        first = group * 2 * inner + (1 if me >= half else 0)
        ready = [first_step + ((k + 1) * units - 1) // rate for k in range(owned)]
        return max(ready[k] + 1 - first - 2 * k for k in range(owned))

    lag_end = max(0, needed(0), needed(count - 1))
    lag_mid = max([lag_end + 1] + [needed(me) for me in range(1, count - 1)])
    return lag_end, lag_mid


def slab_kernel(coef_ref, noise_ref, table_ref, turned_ref, slab_ref, out_ref, coef, wide, spread, zmodes,
                modes, split, lines, total, cubic, parts, landed, noise, halves, coef_sem, noise_sem, mode_recv,
                mode_send, sum_recv, sum_send, first_recv, first_send, second_recv, second_send):
    count = lax.axis_size("my")
    me = lax.axis_index("my")
    row_count = lax.axis_size("mx")
    row = lax.axis_index("mx")
    rep_count = lax.axis_size("rep")
    rep = lax.axis_index("rep")
    planes = noise_ref.shape[0]
    planes_rep = planes * row_count
    row_block = coef_ref.shape[1]
    block = coef_ref.shape[2]
    pair = 2 if rep_count % 2 == 0 else 1
    groups = rep_count // pair
    group = lax.div(rep, pair)
    side = lax.rem(rep, pair)
    spots = [(dg, dh) for dg in range(groups) for dh in range(row_count)]
    offsets = [(dr, dh) for dr in range(rep_count) for dh in range(row_count)]
    full = row_block // 128
    rest = row_block % 128
    pieces = zmodes.shape[1]
    mode_count, point_count = table_ref.shape
    point_block = noise_ref.shape[2]
    width = lines.shape[1] // 2
    units = point_count // width
    chunk = max(c for c in (512, 256, 128) if point_count % c == 0)
    rate = max(1, units // 2)
    modes_step, cubic_step = 2, 6
    half, inner, shared, outer = slab_owners(planes, count)
    lag_end, lag_mid = slab_schedule(planes, count, units, rate, cubic_step)
    tail = max(0, planes - 2)
    up = {"my": me + 1}
    down = {"my": me - 1}
    has_up = me < count - 1
    has_down = me > 0

    barrier = pltpu.get_barrier_semaphore()
    line_peers = [(dh, dm) for dh in range(row_count) for dm in range(count)][1:]
    rep_peers = [(dr, dh) for dr, dh in offsets if dr > 0]
    for dh, dm in line_peers:
        pl.semaphore_signal(
            barrier, inc=1,
            device_id={"mx": lax.rem(row + dh, row_count), "my": lax.rem(me + dm, count)},
            device_id_type=MESH,
        )
    for dr, dh in rep_peers:
        pl.semaphore_signal(
            barrier, inc=1,
            device_id={"rep": lax.rem(rep + dr, rep_count), "mx": lax.rem(row + dh, row_count)},
            device_id_type=MESH,
        )

    def rows(j):
        return pl.ds(pl.multiple_of(j * block, block), block)

    def group_of(p):
        return jnp.minimum(lax.div(p, 2 * inner), half - 1)

    def owner_of(p):
        return jnp.where(lax.rem(p, 2) == 1, half + group_of(p), half - 1 - group_of(p))

    def slot_of(p):
        return lax.div(p - group_of(p) * (2 * inner), 2)

    own_group = jnp.where(me >= half, me - half, half - 1 - me)
    owned = jnp.where(own_group < half - 1, inner, outer)

    def plane_of(k):
        return own_group * (2 * inner) + 2 * k + (me >= half).astype(jnp.int32)

    def mode_copy(p, h, j, target_row, target):
        return pltpu.make_async_remote_copy(
            src_ref=zmodes.at[target_row * planes + p],
            dst_ref=modes.at[slot_of(p), h, :, rows(j)],
            send_sem=mode_send.at[p, target_row],
            recv_sem=mode_recv.at[slot_of(p), h, j],
            device_id={"mx": target_row, "my": target},
            device_id_type=MESH,
        )

    def mode_keep(p):
        return pltpu.make_async_copy(
            zmodes.at[row * planes + p], modes.at[slot_of(p), row, :, rows(me)],
            mode_recv.at[slot_of(p), row, me],
        )

    def plane_at(from_group, from_side, from_row, p):
        return ((from_group * pair + from_side) * row_count + from_row) * planes + p

    def first_copy(p, at, received):
        dg, dh = spots[at]
        target_row = lax.rem(row + dh, row_count)
        if at == 0:
            return pltpu.make_async_copy(
                halves.at[p, row], out_ref.at[plane_at(group, side, row, p)], first_send.at[p, 0]
            )
        if received:
            plane = plane_at(
                lax.rem(group + groups - dg, groups), side, lax.rem(row + row_count - dh, row_count), p
            )
        else:
            plane = plane_at(group, side, row, p)
        return pltpu.make_async_remote_copy(
            src_ref=halves.at[p, target_row],
            dst_ref=out_ref.at[plane],
            send_sem=first_send.at[p, at],
            recv_sem=first_recv.at[p, at],
            device_id={"rep": lax.rem(group + dg, groups) * pair + side, "mx": target_row},
            device_id_type=MESH,
        )

    def second_copy(p, at, received):
        dg, dh = spots[at]
        plane = plane_at(
            lax.rem(group + groups - dg, groups), 1 - side if received else side,
            lax.rem(row + row_count - dh, row_count), p,
        )
        return pltpu.make_async_remote_copy(
            src_ref=halves.at[p, row] if at == 0 else out_ref.at[plane],
            dst_ref=out_ref.at[plane],
            send_sem=second_send.at[p, at],
            recv_sem=second_recv.at[p, at],
            device_id={"rep": group * pair + 1 - side},
            device_id_type=MESH,
        )

    def noise_copy(p):
        slot = lax.rem(p, 2)
        return pltpu.make_async_copy(noise_ref.at[p], noise.at[slot], noise_sem.at[slot])

    def sum_copy(p, j, way, slot):
        return pltpu.make_async_remote_copy(
            src_ref=parts.at[p, :, rows(j)],
            dst_ref=landed.at[p, slot],
            send_sem=sum_send.at[p, way, j],
            recv_sem=sum_recv.at[p, slot],
            device_id=down if way else up,
            device_id_type=MESH,
        )

    strips = block // 16

    def coef_copy(i, part):
        strip = pl.ds(pl.multiple_of(i * 16, 16), 16)
        return pltpu.make_async_copy(coef_ref.at[part, :, strip], coef.at[part], coef_sem.at[part])

    noise_copy(0).start()
    if planes > 1:
        noise_copy(1).start()
    coef_copy(0, 0).start()
    coef_copy(0, 1).start()

    pl.semaphore_wait(barrier, len(line_peers) + len(rep_peers))

    def split_table():
        split[...] = jnp.zeros_like(split)
        for h in range(row_count):
            for part in range(2):
                for t in range(full + (1 if rest else 0)):
                    size = min(128, row_block - t * 128)
                    source = h * row_block + t * 128
                    place = (h * (full + (1 if rest else 0)) + t) * 128 + (part * rest if size < 128 else 0)
                    split[part, place : place + size] = table_ref[source : source + size]

    def contract_strip(i, carry):
        strip = pl.ds(pl.multiple_of(i * 16, 16), 16)
        for part in range(2):
            coef_copy(i, part).wait()
            wide[part] = jnp.dot(
                coef[part].reshape(row_block * 16, coef.shape[3]), slab_ref[...],
                preferred_element_type=jnp.float32,
            )

            @pl.when(i + 1 < strips)
            def _():
                coef_copy(i + 1, part).start()

        for b in range(16):
            for part in range(2):
                for t in range(full):
                    turn = wide[part, pl.ds(t * 2048 + b, 128, stride=16), :].T[:planes_rep]
                    spread[part * full + t, pl.ds(b, planes_rep, stride=16), :] = turn
            if rest:
                both = [wide[part, pl.ds(full * 2048 + b, rest, stride=16), :] for part in range(2)]
                spread[2 * full, pl.ds(b, planes_rep, stride=16), :] = jnp.concatenate(both, 0).T[:planes_rep]
        for t in range(pieces):
            zmodes[:, t, strip, :] = spread[t].reshape(planes_rep, 16, 128).astype(jnp.bfloat16)
        return carry

    def send_modes(i, carry):
        turn = lax.div(i, 2)
        even = min(shared, planes - shared) // 2
        later = turn - even + (0 if shared > planes - shared else shared // 2)
        mixed = lax.div(turn, 2) + lax.rem(turn, 2) * (shared // 2)
        p = 2 * jnp.where(turn < 2 * even, mixed, later) + lax.rem(i, 2)
        target = owner_of(p)
        for dh in range(row_count):
            target_row = lax.rem(row + dh, row_count)
            if dh:
                mode_copy(p, row, me, target_row, target).start()
            else:
                @pl.when(target != me)
                def _():
                    mode_copy(p, row, me, target_row, target).start()

                @pl.when(target == me)
                def _():
                    mode_keep(p).start()
        return carry

    def inside(p):
        return jnp.logical_and(p >= 0, p < planes)

    def span_of(i):
        low = jnp.where(i == planes - 1, tail, i)
        valid = jnp.logical_and(i >= 0, jnp.logical_or(i < tail, i == planes - 1))
        return low, jnp.where(valid, i + 1, low)

    own_points = pl.ds(pl.multiple_of(me * point_block, point_block), point_block)

    def project_noise(p):
        noise_copy(p).wait()
        slot = lax.rem(p, 2)
        step_of = max(c for c in (512, 256, 128) if point_count % c == 0)
        columns = None
        for first in range(0, point_count, step_of):
            span = slice(first, first + step_of)
            field = noise[slot, :, :, span].reshape(2 * point_block, step_of)
            more = lax.dot_general(table_ref[:, span], field, NT, preferred_element_type=jnp.float32)
            columns = more if columns is None else columns + more
        turned = turned_ref[own_points]
        for part in range(2):
            column = columns[:, part * point_block : (part + 1) * point_block].astype(jnp.bfloat16)
            parts[p, part] = jnp.dot(column, turned, preferred_element_type=jnp.float32).astype(
                jnp.bfloat16
            )

        @pl.when(p + 2 < planes)
        def _():
            noise_copy(p + 2).start()

    def wait_modes(k):
        p = plane_of(k)
        for h in range(row_count):
            for j in range(count):
                mine = jnp.logical_and(row == h, me == j)

                @pl.when(mine)
                def _():
                    mode_keep(p).wait()

                @pl.when(jnp.logical_not(mine))
                def _():
                    mode_copy(p, h, j, row, me).wait_recv()

    def cubic_unit(u, carry):
        k = lax.div(u, units)
        at = lax.rem(u, units)

        @pl.when(at == 0)
        def _():
            wait_modes(k)

        span = pl.ds(pl.multiple_of(at * width, width), width)
        for part in range(2):
            field = []
            for h in range(row_count):
                field += [modes[k, h, part * full + t] for t in range(full)]
                if rest:
                    field.append(modes[k, h, 2 * full])
            line = jnp.dot(
                jnp.concatenate(field, 1), split[part, :, span], preferred_element_type=jnp.float32
            )
            lines[:, part * width : (part + 1) * width] = line.astype(jnp.bfloat16)
        columns = None
        for first in range(0, point_count, chunk):
            wave = jnp.dot(
                turned_ref[first : first + chunk], lines[...], preferred_element_type=jnp.float32
            )
            wave_real, wave_imag = wave[:, :width], wave[:, width:]
            density = wave_real * wave_real + wave_imag * wave_imag
            drive = jnp.concatenate(
                [
                    (density * (wave_imag - DAMPING * wave_real)).astype(jnp.bfloat16),
                    (density * (-wave_real - DAMPING * wave_imag)).astype(jnp.bfloat16),
                ],
                1,
            )
            more = jnp.dot(
                table_ref[:, first : first + chunk], drive, preferred_element_type=jnp.float32
            )
            columns = more if columns is None else columns + more
        for part in range(2):
            more = jnp.dot(
                columns[:, part * width : (part + 1) * width].astype(jnp.bfloat16),
                turned_ref[span], preferred_element_type=jnp.float32,
            )

            @pl.when(at == 0)
            def _():
                total[part] = more

            @pl.when(at > 0)
            def _():
                total[part] += more

        @pl.when(at == units - 1)
        def _():
            cubic[k] = total[...].astype(jnp.bfloat16)

        return carry

    def add(p, j, slot):
        both = parts[p, :, rows(j)].astype(jnp.float32) + landed[p, slot].astype(jnp.float32)
        parts[p, :, rows(j)] = both.astype(jnp.bfloat16)

    rise_lag = jnp.where(me == 0, lag_end, lag_mid + me - 1)
    sink_lag = jnp.where(me == count - 1, lag_end, lag_mid + count - 2 - me)
    merge_lag = jnp.minimum(rise_lag, sink_lag)
    done_lag = jnp.maximum(rise_lag, sink_lag)

    def step(s, carry):
        @pl.when(s < planes)
        def _():
            project_noise(s)

        sent = jnp.where(s < shared, s, s - lag_end)
        at_end = jnp.logical_or(me == 0, me == count - 1)
        merging = jnp.where(at_end, sent, s - merge_lag)

        @pl.when(jnp.logical_and(inside(merging), owner_of(merging) == me))
        def _():
            both = parts[merging].astype(jnp.float32) + cubic[slot_of(merging)].astype(jnp.float32)
            parts[merging] = both.astype(jnp.bfloat16)

        low, high = span_of(sent)
        high = jnp.where(jnp.logical_or(s < shared, sent >= shared), high, low)

        @pl.when(me == 0)
        def _():
            for j in range(count - 1, 0, -1):
                def emit(p, carry):
                    sum_copy(p, j, 0, j).start()
                    return carry

                lax.fori_loop(low, high, emit, 0)

        @pl.when(me == count - 1)
        def _():
            for j in range(count - 1):
                def emit(p, carry):
                    sum_copy(p, j, 1, count if j == count - 2 else j).start()
                    return carry

                lax.fori_loop(low, high, emit, 0)

        @pl.when(s == modes_step)
        def _():
            lax.fori_loop(0, strips, contract_strip, 0)
            lax.fori_loop(0, planes, send_modes, 0)

        unit = (s - cubic_step) * rate
        lax.fori_loop(
            jnp.clip(unit, 0, owned * units), jnp.clip(unit + rate, 0, owned * units), cubic_unit, 0
        )

        low, high = span_of(s - rise_lag)
        for far in range(count - 2, 0, -1):
            @pl.when(jnp.logical_and(has_down, me + far <= count - 1))
            def _():
                j = me + far

                def relay(p, carry):
                    sum_copy(p, j, 0, j).wait_recv()
                    add(p, j, j)
                    sum_copy(p, j, 0, j).start()
                    return carry

                lax.fori_loop(low, high, relay, 0)

        low, high = span_of(s - sink_lag)
        for far in range(count - 2, 0, -1):
            @pl.when(jnp.logical_and(has_up, me - far >= 0))
            def _():
                j = me - far

                def relay(p, carry):
                    sum_copy(p, j, 1, j).wait_recv()
                    add(p, j, j)
                    sum_copy(p, j, 1, count if far == 1 else j).start()
                    return carry

                lax.fori_loop(low, high, relay, 0)

        def finish_plane(p, carry):
            @pl.when(has_down)
            def _():
                sum_copy(p, me, 0, me).wait_recv()
                add(p, me, me)

            @pl.when(has_up)
            def _():
                sum_copy(p, me, 1, count).wait_recv()
                add(p, me, count)

            whole = [parts[p, part, rows(me)] for part in range(2)]
            for h in range(row_count):
                for part in range(2):
                    for t in range(full):
                        place = h * row_block + t * 128
                        halves[p, h, part * full + t] = whole[part][:, place : place + 128]
                if rest:
                    place = h * row_block + full * 128
                    halves[p, h, 2 * full] = jnp.concatenate(
                        [whole[part][:, place : place + rest] for part in range(2)], 1
                    )
            for at in range(len(spots) - 1, -1, -1):
                first_copy(p, at, False).start()
            if pair == 2:
                second_copy(p, 0, False).start()
            return carry

        low, high = span_of(s - done_lag)
        lax.fori_loop(low, high, finish_plane, 0)

        def pass_on(p, carry):
            for at in range(1, len(spots)):
                first_copy(p, at, True).wait_recv()
                if pair == 2:
                    second_copy(p, at, False).start()
            return carry

        low, high = span_of(s - done_lag - 1)
        lax.fori_loop(low, high, pass_on, 0)
        return carry

    split_table()
    lax.fori_loop(0, planes + lag_mid + count - 1, step, 0)

    def finish(p, carry):
        for j in range(count):
            @pl.when(j > me)
            def _():
                sum_copy(p, j, 0, j).wait_send()

            @pl.when(j < me)
            def _():
                sum_copy(p, j, 1, j).wait_send()

        target = owner_of(p)
        for dh in range(row_count):
            target_row = lax.rem(row + dh, row_count)
            if dh:
                mode_copy(p, row, me, target_row, target).wait_send()
            else:
                @pl.when(target != me)
                def _():
                    mode_copy(p, row, me, target_row, target).wait_send()

        first_copy(p, 0, False).wait()
        for at in range(len(spots)):
            if at:
                first_copy(p, at, False).wait_send()
            if pair == 2:
                second_copy(p, at, False).wait_send()
                second_copy(p, at, True).wait_recv()
        return carry

    lax.fori_loop(0, planes, finish, 0)


def slab_planes(coefficients, noise_field, mode_table, turned, slab_own):
    count = lax.axis_size("my")
    mode_count = mode_table.shape[0]
    row_count = lax.axis_size("mx")
    rep_count = lax.axis_size("rep")
    _, row_block, block, depth = coefficients.shape
    planes = noise_field.shape[0]
    planes_rep = planes * row_count
    outer = slab_owners(planes, count)[3]
    pieces = 2 * row_block // 128
    places = row_count * pl.cdiv(row_block, 128) * 128
    spots = row_count * (rep_count // (2 if rep_count % 2 == 0 else 1))
    point_block, point_count = noise_field.shape[2:]
    width = max(c for c in (256, 128) if point_count % c == 0)
    lanes = slab_own.shape[1]
    vmem = pl.BlockSpec(memory_space=pltpu.VMEM)
    hbm = pl.BlockSpec(memory_space=pl.ANY)
    dma = pltpu.SemaphoreType.DMA
    flops = 12 * planes * mode_count * point_block * (point_count + mode_count)
    return pl.pallas_call(
        slab_kernel,
        out_shape=jax.ShapeDtypeStruct((planes_rep * rep_count, pieces, block, 128), jnp.bfloat16),
        in_specs=[hbm, hbm, vmem, vmem, vmem],
        out_specs=hbm,
        scratch_shapes=[
            pltpu.VMEM((2, row_block, 16, depth), jnp.bfloat16),
            pltpu.VMEM((2, row_block * 16, lanes), jnp.float32),
            pltpu.VMEM((pieces, planes_rep * 16, 128), jnp.float32),
            pltpu.VMEM((planes_rep, pieces, block, 128), jnp.bfloat16),
            pltpu.VMEM((outer, row_count, pieces, mode_count, 128), jnp.bfloat16),
            pltpu.VMEM((2, places, point_count), jnp.bfloat16),
            pltpu.VMEM((mode_count, 2 * width), jnp.bfloat16),
            pltpu.VMEM((2, mode_count, mode_count), jnp.float32),
            pltpu.VMEM((outer, 2, mode_count, mode_count), jnp.bfloat16),
            pltpu.VMEM((planes, 2, mode_count, mode_count), jnp.bfloat16),
            pltpu.VMEM((planes, count + 1, 2, block, mode_count), jnp.bfloat16),
            pltpu.VMEM((2, 2, point_block, point_count), jnp.bfloat16),
            pltpu.VMEM((planes, row_count, pieces, block, 128), jnp.bfloat16),
            dma((2,)),
            dma((2,)),
            dma((outer, row_count, count)),
            dma((planes, row_count)),
            dma((planes, count + 1)),
            dma((planes, 2, count)),
            dma((planes, spots)),
            dma((planes, spots)),
            dma((planes, spots)),
            dma((planes, spots)),
        ],
        compiler_params=pltpu.CompilerParams(
            collective_id=0, has_side_effects=True, vmem_limit_bytes=60 * 1024 * 1024
        ),
        cost_estimate=pl.CostEstimate(
            flops=flops, bytes_accessed=noise_field.size * 2, transcendentals=0
        ),
    )(coefficients, noise_field, mode_table, turned, slab_own)


def update_kernel(grid_ref, slab_ref, out_ref, wide, lines):
    planes, pieces, strip, lanes = grid_ref.shape
    _, row_block, _, own_block = out_ref.shape
    full = row_block // lanes
    rest = row_block % lanes
    for t in range(pieces):
        wide[t] = grid_ref[:, t].astype(jnp.float32).reshape(planes * strip, lanes)
    for t in range(pieces):
        for b in range(0, strip, 2):
            pair = [
                wide[t, pl.ds(b + e, planes, stride=strip), :].astype(jnp.bfloat16) for e in range(2)
            ]
            both = jnp.dot(
                slab_ref[...], jnp.concatenate(pair, 1), preferred_element_type=jnp.float32
            )
            for e in range(2):
                turn = both[:, e * lanes : (e + 1) * lanes].T
                if t < 2 * full:
                    first = (t % full) * lanes * strip + b + e
                    lines[t // full, pl.ds(first, lanes, stride=strip), :] = turn
                else:
                    first = full * lanes * strip + b + e
                    for part in range(2):
                        lines[part, pl.ds(first, rest, stride=strip), :] = turn[
                            part * rest : (part + 1) * rest
                        ]
    for part in range(2):
        out_ref[part] = (
            lines[part, :, :own_block].reshape(row_block, strip, own_block).astype(jnp.bfloat16)
        )


def update_planes(plane_grid, slab_back, row_block):
    planes, pieces, block, lanes = plane_grid.shape
    own_block = slab_back.shape[0]
    strip = 16
    slab = jnp.pad(slab_back, ((0, lanes - own_block), (0, 0)))
    return pl.pallas_call(
        update_kernel,
        grid=(block // strip,),
        out_shape=jax.ShapeDtypeStruct((2, row_block, block, own_block), jnp.bfloat16),
        in_specs=[
            pl.BlockSpec((planes, pieces, strip, lanes), lambda b: (0, 0, b, 0)),
            pl.BlockSpec((lanes, planes), lambda b: (0, 0)),
        ],
        out_specs=pl.BlockSpec((2, row_block, strip, own_block), lambda b: (0, 0, b, 0)),
        scratch_shapes=[
            pltpu.VMEM((pieces, planes * strip, lanes), jnp.float32),
            pltpu.VMEM((2, row_block * strip, lanes), jnp.float32),
        ],
        compiler_params=pltpu.CompilerParams(vmem_limit_bytes=60 * 1024 * 1024),
        cost_estimate=pl.CostEstimate(
            flops=4 * planes * row_block * block * own_block, bytes_accessed=plane_grid.size * 2,
            transcendentals=0,
        ),
    )(plane_grid, slab)


def body(coefficients, noise_field, mode_table):
    rep_index = lax.axis_index("rep")
    rep_count = lax.axis_size("rep")
    row_count = lax.axis_size("mx")
    col_count = lax.axis_size("my")
    planes_dev = noise_field.shape[0]
    planes_rep = planes_dev * row_count
    planes_all = planes_rep * rep_count
    mode_count = mode_table.shape[0]
    point_count = mode_table.shape[1]
    slab_first = point_count // 2 - planes_all // 2
    row_block = mode_count // row_count
    col_block = mode_count // col_count
    point_block = point_count // col_count
    own_block = mode_count // rep_count
    if (
        col_block % 16 or row_block % 16 or point_block % 128 or mode_count % 128
        or row_block % 64 or col_count < 2 or col_count % 2 or planes_dev % (2 * col_count)
        or planes_rep > 128 or planes_rep % 8 or planes_all % 8 or own_block > 128
    ):
        return plain_body(coefficients, noise_field, mode_table)
    slab_own = lax.dynamic_slice_in_dim(
        mode_table, slab_first + rep_index * planes_rep, planes_rep, 1
    )
    slab_own = jnp.pad(slab_own, ((0, 0), (0, 128 - planes_rep)))
    plane_grid = slab_planes(coefficients, noise_field, mode_table, mode_table.T, slab_own)
    slab_back = lax.dynamic_slice_in_dim(mode_table, rep_index * own_block, own_block, 0)[
        :, slab_first : slab_first + planes_all
    ]
    return update_planes(plane_grid, slab_back, row_block)


def solution(mesh):
    in_specs = (P(None, "mx", "my", None), P(("rep", "mx"), None, "my", None), P())
    out_specs = P(None, "mx", "my", "rep")
    return jax.shard_map(body, mesh=mesh, in_specs=in_specs, out_specs=out_specs, check_vma=False)
```

```python
import jax
import jax.numpy as jnp
from jax import lax
from jax.experimental import pallas as pl
from jax.experimental.pallas import tpu as pltpu
from jax.sharding import PartitionSpec as P

DAMPING = 0.25
MESH = pl.DeviceIdType.MESH
NT = (((1,), (1,)), ((), ()))


def plain_body(coefficients, noise_field, mode_table):
    rep_index = lax.axis_index("rep")
    col_index = lax.axis_index("my")
    rep_count = lax.axis_size("rep")
    row_count = lax.axis_size("mx")
    col_count = lax.axis_size("my")
    planes_dev = noise_field.shape[0]
    planes_rep = planes_dev * row_count
    planes_all = planes_rep * rep_count
    mode_count = mode_table.shape[0]
    point_count = mode_table.shape[1]
    slab_first = point_count // 2 - planes_all // 2
    row_block = mode_count // row_count
    col_block = mode_count // col_count
    point_block = point_count // col_count
    own_block = mode_count // rep_count
    slab_own = lax.dynamic_slice_in_dim(
        mode_table, slab_first + rep_index * planes_rep, planes_rep, 1
    )
    zmodes = jnp.einsum(
        "pabk,kz->zpba", coefficients, slab_own, preferred_element_type=jnp.float32
    ).astype(jnp.bfloat16)
    zmodes = zmodes.reshape(planes_rep, 2, col_block * row_block)
    spread = lax.all_to_all(zmodes, "mx", split_axis=0, concat_axis=2, tiled=True)
    grouped = spread.reshape(planes_dev, 2, row_count, col_block, row_block)
    tiled_table = mode_table.reshape(row_count, row_block, point_count)
    own_points = lax.dynamic_slice_in_dim(tiled_table, col_index * point_block, point_block, 2)
    block_part = jnp.einsum(
        "zpsal,slx->zpax",
        lax.all_gather(grouped, "my", axis=3, tiled=True),
        own_points,
        preferred_element_type=jnp.float32,
    ).astype(jnp.bfloat16)
    wave_field = jnp.einsum(
        "zpax,ay->zpxy", block_part, mode_table, preferred_element_type=jnp.float32
    )
    wave_real = wave_field[:, 0]
    wave_imag = wave_field[:, 1]
    density = wave_real * wave_real + wave_imag * wave_imag
    noise_wide = noise_field.astype(jnp.float32)
    drive_term = jnp.stack(
        [
            density * (wave_imag - DAMPING * wave_real) + noise_wide[:, 0],
            density * (-wave_real - DAMPING * wave_imag) + noise_wide[:, 1],
        ],
        1,
    ).astype(jnp.bfloat16)
    proj_columns = jnp.einsum(
        "zpxy,ny->zpnx", drive_term, mode_table, preferred_element_type=jnp.float32
    ).astype(jnp.bfloat16)
    block_part = lax.all_to_all(proj_columns, "my", split_axis=2, concat_axis=3, tiled=True)
    folded = jnp.einsum(
        "zpax,slx->zpsal", block_part, tiled_table, preferred_element_type=jnp.float32
    ).astype(jnp.bfloat16)
    proj_rows = folded.reshape(
        block_part.shape[0], block_part.shape[1], row_count * col_block * row_block
    )
    gathered_rows = lax.all_to_all(proj_rows, "mx", split_axis=2, concat_axis=0, tiled=True)
    slab_back = lax.dynamic_slice_in_dim(mode_table, rep_index * own_block, own_block, 0)[
        :, slab_first : slab_first + planes_all
    ]
    portion = lax.all_gather(gathered_rows, "rep", axis=0, tiled=True)
    plane_grid = portion.reshape(portion.shape[0], 2, col_block, row_block)
    summed = jnp.einsum("zpba,nz->pabn", plane_grid, slab_back, preferred_element_type=jnp.float32)
    return summed.astype(jnp.bfloat16)

def slab_owners(planes, count):
    half = count // 2
    inner = max(1, planes // (2 * count))
    shared = 2 * inner * (half - 1)
    return half, inner, shared, (planes - shared) // 2


def slab_schedule(planes, count, units, rate, first_step):
    half, inner, shared, outer = slab_owners(planes, count)

    def needed(me):
        group = me - half if me >= half else half - 1 - me
        owned = inner if group < half - 1 else outer
        first = group * 2 * inner + (1 if me >= half else 0)
        ready = [first_step + ((k + 1) * units - 1) // rate for k in range(owned)]
        return max(ready[k] + 1 - first - 2 * k for k in range(owned))

    lag_end = max(0, needed(0), needed(count - 1))
    lag_mid = max([lag_end + 1] + [needed(me) for me in range(1, count - 1)])
    return lag_end, lag_mid


def slab_kernel(coef_ref, noise_ref, table_ref, out_ref, back_ref, coef, wide, spread, zmodes, modes, split,
                turned_ref, slab_ref, lines, total, cubic, parts, landed, noise, halves, coef_sem, noise_sem, mode_recv,
                mode_send, sum_recv, sum_send, first_recv, first_send, second_recv, second_send):
    count = lax.axis_size("my")
    me = lax.axis_index("my")
    row_count = lax.axis_size("mx")
    row = lax.axis_index("mx")
    rep_count = lax.axis_size("rep")
    rep = lax.axis_index("rep")
    planes = noise_ref.shape[0]
    planes_rep = planes * row_count
    row_block = coef_ref.shape[1]
    block = coef_ref.shape[2]
    pair = 2 if rep_count % 2 == 0 else 1
    groups = rep_count // pair
    group = lax.div(rep, pair)
    side = lax.rem(rep, pair)
    spots = [(dg, dh) for dg in range(groups) for dh in range(row_count)]
    offsets = [(dr, dh) for dr in range(rep_count) for dh in range(row_count)]
    full = row_block // 128
    rest = row_block % 128
    pieces = zmodes.shape[1]
    mode_count, point_count = table_ref.shape
    point_block = noise_ref.shape[2]
    width = lines.shape[1] // 2
    units = point_count // width
    chunk = max(c for c in (512, 256, 128) if point_count % c == 0)
    rate = max(1, units // 2)
    modes_step, cubic_step = 2, 5
    half, inner, shared, outer = slab_owners(planes, count)
    lag_end, lag_mid = slab_schedule(planes, count, units, rate, cubic_step)
    tail = max(0, planes - 2)
    up = {"my": me + 1}
    down = {"my": me - 1}
    has_up = me < count - 1
    has_down = me > 0

    barrier = pltpu.get_barrier_semaphore()
    line_peers = [(dh, dm) for dh in range(row_count) for dm in range(count)][1:]
    rep_peers = [(dr, dh) for dr, dh in offsets if dr > 0]
    for dh, dm in line_peers:
        pl.semaphore_signal(
            barrier, inc=1,
            device_id={"mx": lax.rem(row + dh, row_count), "my": lax.rem(me + dm, count)},
            device_id_type=MESH,
        )
    for dr, dh in rep_peers:
        pl.semaphore_signal(
            barrier, inc=1,
            device_id={"rep": lax.rem(rep + dr, rep_count), "mx": lax.rem(row + dh, row_count)},
            device_id_type=MESH,
        )

    def rows(j):
        return pl.ds(pl.multiple_of(j * block, block), block)

    def group_of(p):
        return jnp.minimum(lax.div(p, 2 * inner), half - 1)

    def owner_of(p):
        return jnp.where(lax.rem(p, 2) == 1, half + group_of(p), half - 1 - group_of(p))

    def slot_of(p):
        return lax.div(p - group_of(p) * (2 * inner), 2)

    own_group = jnp.where(me >= half, me - half, half - 1 - me)
    owned = jnp.where(own_group < half - 1, inner, outer)

    def plane_of(k):
        return own_group * (2 * inner) + 2 * k + (me >= half).astype(jnp.int32)

    def mode_copy(p, h, j, target_row, target):
        return pltpu.make_async_remote_copy(
            src_ref=zmodes.at[target_row * planes + p],
            dst_ref=modes.at[slot_of(p), h, :, rows(j)],
            send_sem=mode_send.at[p, target_row],
            recv_sem=mode_recv.at[slot_of(p), h, j],
            device_id={"mx": target_row, "my": target},
            device_id_type=MESH,
        )

    def mode_keep(p):
        return pltpu.make_async_copy(
            zmodes.at[row * planes + p], modes.at[slot_of(p), row, :, rows(me)],
            mode_recv.at[slot_of(p), row, me],
        )

    def plane_at(from_group, from_side, from_row, p):
        return ((from_group * pair + from_side) * row_count + from_row) * planes + p

    def first_copy(p, at, received):
        dg, dh = spots[at]
        target_row = lax.rem(row + dh, row_count)
        if at == 0:
            return pltpu.make_async_copy(
                halves.at[p, row], out_ref.at[plane_at(group, side, row, p)], first_send.at[p, 0]
            )
        if received:
            plane = plane_at(
                lax.rem(group + groups - dg, groups), side, lax.rem(row + row_count - dh, row_count), p
            )
        else:
            plane = plane_at(group, side, row, p)
        return pltpu.make_async_remote_copy(
            src_ref=halves.at[p, target_row],
            dst_ref=out_ref.at[plane],
            send_sem=first_send.at[p, at],
            recv_sem=first_recv.at[p, at],
            device_id={"rep": lax.rem(group + dg, groups) * pair + side, "mx": target_row},
            device_id_type=MESH,
        )

    def second_copy(p, at, received):
        dg, dh = spots[at]
        plane = plane_at(
            lax.rem(group + groups - dg, groups), 1 - side if received else side,
            lax.rem(row + row_count - dh, row_count), p,
        )
        return pltpu.make_async_remote_copy(
            src_ref=halves.at[p, row] if at == 0 else out_ref.at[plane],
            dst_ref=out_ref.at[plane],
            send_sem=second_send.at[p, at],
            recv_sem=second_recv.at[p, at],
            device_id={"rep": group * pair + 1 - side},
            device_id_type=MESH,
        )

    def noise_copy(p):
        slot = lax.rem(p, 2)
        return pltpu.make_async_copy(noise_ref.at[p], noise.at[slot], noise_sem.at[slot])

    def sum_copy(p, j, way, slot):
        return pltpu.make_async_remote_copy(
            src_ref=parts.at[p, :, rows(j)],
            dst_ref=landed.at[p, slot],
            send_sem=sum_send.at[p, way, j],
            recv_sem=sum_recv.at[p, slot],
            device_id=down if way else up,
            device_id_type=MESH,
        )

    strips = block // 16

    def coef_copy(i, part):
        strip = pl.ds(pl.multiple_of(i * 16, 16), 16)
        return pltpu.make_async_copy(coef_ref.at[part, :, strip], coef.at[part], coef_sem.at[part])

    noise_copy(0).start()
    if planes > 1:
        noise_copy(1).start()
    coef_copy(0, 0).start()
    coef_copy(0, 1).start()

    def selected(source, offset, wanted):
        shape = (source.shape[1], 128)
        source_at = lax.broadcasted_iota(jnp.int32, shape, 0)
        target_at = lax.broadcasted_iota(jnp.int32, shape, 1)
        chosen = jnp.logical_and(source_at == target_at + offset, target_at < wanted)
        return jnp.dot(
            source, chosen.astype(jnp.float32).astype(jnp.bfloat16), preferred_element_type=jnp.float32
        ).astype(jnp.bfloat16)

    def prepare_tables():
        planes_all = planes_rep * rep_count
        slab_first = point_count // 2 - planes_all // 2
        base = slab_first // 128 * 128
        window = slice(base, pl.cdiv(slab_first + planes_all, 128) * 128)
        slab_ref[...] = selected(table_ref[:, window], slab_first - base + rep * planes_rep, planes_rep)
        own_block = mode_count // rep_count
        own_rows = pl.ds(pl.multiple_of(rep * own_block, own_block), own_block)
        back = selected(table_ref[own_rows, window], slab_first - base, planes_all)
        back_ref[...] = jnp.concatenate([back, jnp.zeros((128 - own_block, 128), jnp.bfloat16)], 0)
        for first in range(0, point_count, 128):
            turned_ref[first : first + 128] = table_ref[:, first : first + 128].T
        split[...] = jnp.zeros_like(split)
        for h in range(row_count):
            for part in range(2):
                for t in range(full + (1 if rest else 0)):
                    size = min(128, row_block - t * 128)
                    source = h * row_block + t * 128
                    place = (h * (full + (1 if rest else 0)) + t) * 128 + (part * rest if size < 128 else 0)
                    split[part, place : place + size] = table_ref[source : source + size]

    def contract_strip(i, carry):
        strip = pl.ds(pl.multiple_of(i * 16, 16), 16)
        for part in range(2):
            coef_copy(i, part).wait()
            wide[part] = jnp.dot(
                coef[part].reshape(row_block * 16, coef.shape[3]), slab_ref[...],
                preferred_element_type=jnp.float32,
            )

            @pl.when(i + 1 < strips)
            def _():
                coef_copy(i + 1, part).start()

        for b in range(16):
            for part in range(2):
                for t in range(full):
                    turn = wide[part, pl.ds(t * 2048 + b, 128, stride=16), :].T[:planes_rep]
                    spread[part * full + t, pl.ds(b, planes_rep, stride=16), :] = turn
            if rest:
                both = [wide[part, pl.ds(full * 2048 + b, rest, stride=16), :] for part in range(2)]
                spread[2 * full, pl.ds(b, planes_rep, stride=16), :] = jnp.concatenate(both, 0).T[:planes_rep]
        for t in range(pieces):
            zmodes[:, t, strip, :] = spread[t].reshape(planes_rep, 16, 128).astype(jnp.bfloat16)
        return carry

    def send_modes(i, carry):
        turn = lax.div(i, 2)
        even = min(shared, planes - shared) // 2
        later = turn - even + (0 if shared > planes - shared else shared // 2)
        mixed = lax.div(turn, 2) + lax.rem(turn, 2) * (shared // 2)
        p = 2 * jnp.where(turn < 2 * even, mixed, later) + lax.rem(i, 2)
        target = owner_of(p)
        for dh in range(row_count):
            target_row = lax.rem(row + dh, row_count)
            if dh:
                mode_copy(p, row, me, target_row, target).start()
            else:
                @pl.when(target != me)
                def _():
                    mode_copy(p, row, me, target_row, target).start()

                @pl.when(target == me)
                def _():
                    mode_keep(p).start()
        return carry

    def inside(p):
        return jnp.logical_and(p >= 0, p < planes)

    def span_of(i):
        low = jnp.where(i == planes - 1, tail, i)
        valid = jnp.logical_and(i >= 0, jnp.logical_or(i < tail, i == planes - 1))
        return low, jnp.where(valid, i + 1, low)

    own_points = pl.ds(pl.multiple_of(me * point_block, point_block), point_block)

    def project_noise(p):
        noise_copy(p).wait()
        slot = lax.rem(p, 2)
        step_of = max(c for c in (512, 256, 128) if point_count % c == 0)
        columns = None
        for first in range(0, point_count, step_of):
            span = slice(first, first + step_of)
            field = noise[slot, :, :, span].reshape(2 * point_block, step_of)
            more = lax.dot_general(table_ref[:, span], field, NT, preferred_element_type=jnp.float32)
            columns = more if columns is None else columns + more
        own_table = table_ref[:, own_points]
        for part in range(2):
            column = columns[:, part * point_block : (part + 1) * point_block].astype(jnp.bfloat16)
            parts[p, part] = lax.dot_general(
                column, own_table, NT, preferred_element_type=jnp.float32
            ).astype(jnp.bfloat16)

        @pl.when(p + 2 < planes)
        def _():
            noise_copy(p + 2).start()

    def wait_modes(k):
        p = plane_of(k)
        for h in range(row_count):
            for j in range(count):
                mine = jnp.logical_and(row == h, me == j)

                @pl.when(mine)
                def _():
                    mode_keep(p).wait()

                @pl.when(jnp.logical_not(mine))
                def _():
                    mode_copy(p, h, j, row, me).wait_recv()

    def cubic_unit(u, carry):
        k = lax.div(u, units)
        at = lax.rem(u, units)

        @pl.when(at == 0)
        def _():
            wait_modes(k)

        span = pl.ds(pl.multiple_of(at * width, width), width)
        for part in range(2):
            field = []
            for h in range(row_count):
                field += [modes[k, h, part * full + t] for t in range(full)]
                if rest:
                    field.append(modes[k, h, 2 * full])
            line = jnp.dot(
                jnp.concatenate(field, 1), split[part, :, span], preferred_element_type=jnp.float32
            )
            lines[:, part * width : (part + 1) * width] = line.astype(jnp.bfloat16)
        columns = None
        for first in range(0, point_count, chunk):
            wave = jnp.dot(
                turned_ref[first : first + chunk], lines[...], preferred_element_type=jnp.float32
            )
            wave_real, wave_imag = wave[:, :width], wave[:, width:]
            density = wave_real * wave_real + wave_imag * wave_imag
            drive = jnp.concatenate(
                [
                    (density * (wave_imag - DAMPING * wave_real)).astype(jnp.bfloat16),
                    (density * (-wave_real - DAMPING * wave_imag)).astype(jnp.bfloat16),
                ],
                1,
            )
            more = jnp.dot(
                table_ref[:, first : first + chunk], drive, preferred_element_type=jnp.float32
            )
            columns = more if columns is None else columns + more
        for part in range(2):
            more = jnp.dot(
                columns[:, part * width : (part + 1) * width].astype(jnp.bfloat16),
                turned_ref[span], preferred_element_type=jnp.float32,
            )

            @pl.when(at == 0)
            def _():
                total[part] = more

            @pl.when(at > 0)
            def _():
                total[part] += more

        @pl.when(at == units - 1)
        def _():
            cubic[k] = total[...].astype(jnp.bfloat16)

        return carry

    def add(p, j, slot):
        both = parts[p, :, rows(j)].astype(jnp.float32) + landed[p, slot].astype(jnp.float32)
        parts[p, :, rows(j)] = both.astype(jnp.bfloat16)

    rise_lag = jnp.where(me == 0, lag_end, lag_mid + me - 1)
    sink_lag = jnp.where(me == count - 1, lag_end, lag_mid + count - 2 - me)
    merge_lag = jnp.minimum(rise_lag, sink_lag)
    done_lag = jnp.maximum(rise_lag, sink_lag)

    def step(s, carry):
        sent = jnp.where(s < shared, s, s - lag_end)
        at_end = jnp.logical_or(me == 0, me == count - 1)
        merging = jnp.where(at_end, sent, s - merge_lag)

        @pl.when(jnp.logical_and(inside(merging), owner_of(merging) == me))
        def _():
            both = parts[merging].astype(jnp.float32) + cubic[slot_of(merging)].astype(jnp.float32)
            parts[merging] = both.astype(jnp.bfloat16)

        low, high = span_of(sent)
        high = jnp.where(jnp.logical_or(s < shared, sent >= shared), high, low)

        @pl.when(me == 0)
        def _():
            for j in range(count - 1, 0, -1):
                def emit(p, carry):
                    sum_copy(p, j, 0, j).start()
                    return carry

                lax.fori_loop(low, high, emit, 0)

        @pl.when(me == count - 1)
        def _():
            for j in range(count - 1):
                def emit(p, carry):
                    sum_copy(p, j, 1, count if j == count - 2 else j).start()
                    return carry

                lax.fori_loop(low, high, emit, 0)

        @pl.when(s == modes_step)
        def _():
            prepare_tables()
            lax.fori_loop(0, strips, contract_strip, 0)
            lax.fori_loop(0, planes, send_modes, 0)

        @pl.when(s + 1 < planes)
        def _():
            project_noise(s + 1)

        unit = (s - cubic_step) * rate
        lax.fori_loop(
            jnp.clip(unit, 0, owned * units), jnp.clip(unit + rate, 0, owned * units), cubic_unit, 0
        )

        low, high = span_of(s - rise_lag)
        for far in range(count - 2, 0, -1):
            @pl.when(jnp.logical_and(has_down, me + far <= count - 1))
            def _():
                j = me + far

                def relay(p, carry):
                    sum_copy(p, j, 0, j).wait_recv()
                    add(p, j, j)
                    sum_copy(p, j, 0, j).start()
                    return carry

                lax.fori_loop(low, high, relay, 0)

        low, high = span_of(s - sink_lag)
        for far in range(count - 2, 0, -1):
            @pl.when(jnp.logical_and(has_up, me - far >= 0))
            def _():
                j = me - far

                def relay(p, carry):
                    sum_copy(p, j, 1, j).wait_recv()
                    add(p, j, j)
                    sum_copy(p, j, 1, count if far == 1 else j).start()
                    return carry

                lax.fori_loop(low, high, relay, 0)

        def finish_plane(p, carry):
            @pl.when(has_down)
            def _():
                sum_copy(p, me, 0, me).wait_recv()
                add(p, me, me)

            @pl.when(has_up)
            def _():
                sum_copy(p, me, 1, count).wait_recv()
                add(p, me, count)

            whole = [parts[p, part, rows(me)] for part in range(2)]
            for h in range(row_count):
                for part in range(2):
                    for t in range(full):
                        place = h * row_block + t * 128
                        halves[p, h, part * full + t] = whole[part][:, place : place + 128]
                if rest:
                    place = h * row_block + full * 128
                    halves[p, h, 2 * full] = jnp.concatenate(
                        [whole[part][:, place : place + rest] for part in range(2)], 1
                    )
            for at in range(len(spots) - 1, -1, -1):
                first_copy(p, at, False).start()
            if pair == 2:
                second_copy(p, 0, False).start()
            return carry

        low, high = span_of(s - done_lag)
        lax.fori_loop(low, high, finish_plane, 0)

        def pass_on(p, carry):
            for at in range(1, len(spots)):
                first_copy(p, at, True).wait_recv()
                if pair == 2:
                    second_copy(p, at, False).start()
            return carry

        low, high = span_of(s - done_lag - 1)
        lax.fori_loop(low, high, pass_on, 0)
        return carry

    project_noise(0)
    pl.semaphore_wait(barrier, len(line_peers) + len(rep_peers))
    lax.fori_loop(0, planes + lag_mid + count - 1, step, 0)

    def finish(p, carry):
        for j in range(count):
            @pl.when(j > me)
            def _():
                sum_copy(p, j, 0, j).wait_send()

            @pl.when(j < me)
            def _():
                sum_copy(p, j, 1, j).wait_send()

        target = owner_of(p)
        for dh in range(row_count):
            target_row = lax.rem(row + dh, row_count)
            if dh:
                mode_copy(p, row, me, target_row, target).wait_send()
            else:
                @pl.when(target != me)
                def _():
                    mode_copy(p, row, me, target_row, target).wait_send()

        first_copy(p, 0, False).wait()
        for at in range(len(spots)):
            if at:
                first_copy(p, at, False).wait_send()
            if pair == 2:
                second_copy(p, at, False).wait_send()
                second_copy(p, at, True).wait_recv()
        return carry

    lax.fori_loop(0, planes, finish, 0)


def slab_planes(coefficients, noise_field, mode_table):
    count = lax.axis_size("my")
    mode_count = mode_table.shape[0]
    row_count = lax.axis_size("mx")
    rep_count = lax.axis_size("rep")
    _, row_block, block, depth = coefficients.shape
    planes = noise_field.shape[0]
    planes_rep = planes * row_count
    outer = slab_owners(planes, count)[3]
    pieces = 2 * row_block // 128
    places = row_count * pl.cdiv(row_block, 128) * 128
    spots = row_count * (rep_count // (2 if rep_count % 2 == 0 else 1))
    point_block, point_count = noise_field.shape[2:]
    width = max(c for c in (256, 128) if point_count % c == 0)
    vmem = pl.BlockSpec(memory_space=pltpu.VMEM)
    hbm = pl.BlockSpec(memory_space=pl.ANY)
    dma = pltpu.SemaphoreType.DMA
    flops = 12 * planes * mode_count * point_block * (point_count + mode_count)
    return pl.pallas_call(
        slab_kernel,
        out_shape=(
            jax.ShapeDtypeStruct((planes_rep * rep_count, pieces, block, 128), jnp.bfloat16),
            jax.ShapeDtypeStruct((128, 128), jnp.bfloat16),
        ),
        in_specs=[hbm, hbm, vmem],
        out_specs=(hbm, vmem),
        scratch_shapes=[
            pltpu.VMEM((2, row_block, 16, depth), jnp.bfloat16),
            pltpu.VMEM((2, row_block * 16, 128), jnp.float32),
            pltpu.VMEM((pieces, planes_rep * 16, 128), jnp.float32),
            pltpu.VMEM((planes_rep, pieces, block, 128), jnp.bfloat16),
            pltpu.VMEM((outer, row_count, pieces, mode_count, 128), jnp.bfloat16),
            pltpu.VMEM((2, places, point_count), jnp.bfloat16),
            pltpu.VMEM((point_count, mode_count), jnp.bfloat16),
            pltpu.VMEM((depth, 128), jnp.bfloat16),
            pltpu.VMEM((mode_count, 2 * width), jnp.bfloat16),
            pltpu.VMEM((2, mode_count, mode_count), jnp.float32),
            pltpu.VMEM((outer, 2, mode_count, mode_count), jnp.bfloat16),
            pltpu.VMEM((planes, 2, mode_count, mode_count), jnp.bfloat16),
            pltpu.VMEM((planes, count + 1, 2, block, mode_count), jnp.bfloat16),
            pltpu.VMEM((2, 2, point_block, point_count), jnp.bfloat16),
            pltpu.VMEM((planes, row_count, pieces, block, 128), jnp.bfloat16),
            dma((2,)),
            dma((2,)),
            dma((outer, row_count, count)),
            dma((planes, row_count)),
            dma((planes, count + 1)),
            dma((planes, 2, count)),
            dma((planes, spots)),
            dma((planes, spots)),
            dma((planes, spots)),
            dma((planes, spots)),
        ],
        compiler_params=pltpu.CompilerParams(
            collective_id=0, has_side_effects=True, vmem_limit_bytes=60 * 1024 * 1024
        ),
        cost_estimate=pl.CostEstimate(
            flops=flops, bytes_accessed=noise_field.size * 2, transcendentals=0
        ),
    )(coefficients, noise_field, mode_table)


def update_kernel(grid_ref, slab_ref, out_ref, wide, lines):
    planes, pieces, strip, lanes = grid_ref.shape
    _, row_block, _, own_block = out_ref.shape
    full = row_block // lanes
    rest = row_block % lanes
    for t in range(pieces):
        wide[t] = grid_ref[:, t].astype(jnp.float32).reshape(planes * strip, lanes)
    for t in range(pieces):
        for b in range(0, strip, 2):
            pair = [
                wide[t, pl.ds(b + e, planes, stride=strip), :].astype(jnp.bfloat16) for e in range(2)
            ]
            both = jnp.dot(
                slab_ref[...], jnp.concatenate(pair, 1), preferred_element_type=jnp.float32
            )
            for e in range(2):
                turn = both[:, e * lanes : (e + 1) * lanes].T
                if t < 2 * full:
                    first = (t % full) * lanes * strip + b + e
                    lines[t // full, pl.ds(first, lanes, stride=strip), :] = turn
                else:
                    first = full * lanes * strip + b + e
                    for part in range(2):
                        lines[part, pl.ds(first, rest, stride=strip), :] = turn[
                            part * rest : (part + 1) * rest
                        ]
    for part in range(2):
        out_ref[part] = (
            lines[part, :, :own_block].reshape(row_block, strip, own_block).astype(jnp.bfloat16)
        )


def update_planes(plane_grid, slab_back, row_block, own_block):
    planes, pieces, block, lanes = plane_grid.shape
    strip = 16
    return pl.pallas_call(
        update_kernel,
        grid=(block // strip,),
        out_shape=jax.ShapeDtypeStruct((2, row_block, block, own_block), jnp.bfloat16),
        in_specs=[
            pl.BlockSpec((planes, pieces, strip, lanes), lambda b: (0, 0, b, 0)),
            pl.BlockSpec((lanes, planes), lambda b: (0, 0)),
        ],
        out_specs=pl.BlockSpec((2, row_block, strip, own_block), lambda b: (0, 0, b, 0)),
        scratch_shapes=[
            pltpu.VMEM((pieces, planes * strip, lanes), jnp.float32),
            pltpu.VMEM((2, row_block * strip, lanes), jnp.float32),
        ],
        compiler_params=pltpu.CompilerParams(vmem_limit_bytes=60 * 1024 * 1024),
        cost_estimate=pl.CostEstimate(
            flops=4 * planes * row_block * block * own_block, bytes_accessed=plane_grid.size * 2,
            transcendentals=0,
        ),
    )(plane_grid, slab_back)


def body(coefficients, noise_field, mode_table):
    rep_count = lax.axis_size("rep")
    row_count = lax.axis_size("mx")
    col_count = lax.axis_size("my")
    planes_dev = noise_field.shape[0]
    planes_rep = planes_dev * row_count
    planes_all = planes_rep * rep_count
    mode_count = mode_table.shape[0]
    point_count = mode_table.shape[1]
    row_block = mode_count // row_count
    col_block = mode_count // col_count
    point_block = point_count // col_count
    own_block = mode_count // rep_count
    if (
        col_block % 16 or row_block % 16 or point_block % 128 or mode_count % 128
        or row_block % 64 or col_count < 2 or col_count % 2 or planes_dev % (2 * col_count)
        or planes_rep % 8 or planes_all != 128 or own_block > 128 or own_block % 16
    ):
        return plain_body(coefficients, noise_field, mode_table)
    plane_grid, slab_back = slab_planes(coefficients, noise_field, mode_table)
    return update_planes(plane_grid, slab_back, row_block, own_block)


def solution(mesh):
    in_specs = (P(None, "mx", "my", None), P(("rep", "mx"), None, "my", None), P())
    out_specs = P(None, "mx", "my", "rep")
    return jax.shard_map(body, mesh=mesh, in_specs=in_specs, out_specs=out_specs, check_vma=False)
```

```python
import jax
import jax.numpy as jnp
from jax import lax
from jax.experimental import pallas as pl
from jax.experimental.pallas import tpu as pltpu
from jax.sharding import PartitionSpec as P

DAMPING = 0.25
MESH = pl.DeviceIdType.MESH
NT = (((1,), (1,)), ((), ()))


def plain_body(coefficients, noise_field, mode_table):
    rep_index = lax.axis_index("rep")
    col_index = lax.axis_index("my")
    rep_count = lax.axis_size("rep")
    row_count = lax.axis_size("mx")
    col_count = lax.axis_size("my")
    planes_dev = noise_field.shape[0]
    planes_rep = planes_dev * row_count
    planes_all = planes_rep * rep_count
    mode_count = mode_table.shape[0]
    point_count = mode_table.shape[1]
    slab_first = point_count // 2 - planes_all // 2
    row_block = mode_count // row_count
    col_block = mode_count // col_count
    point_block = point_count // col_count
    own_block = mode_count // rep_count
    slab_own = lax.dynamic_slice_in_dim(
        mode_table, slab_first + rep_index * planes_rep, planes_rep, 1
    )
    zmodes = jnp.einsum(
        "pabk,kz->zpba", coefficients, slab_own, preferred_element_type=jnp.float32
    ).astype(jnp.bfloat16)
    zmodes = zmodes.reshape(planes_rep, 2, col_block * row_block)
    spread = lax.all_to_all(zmodes, "mx", split_axis=0, concat_axis=2, tiled=True)
    grouped = spread.reshape(planes_dev, 2, row_count, col_block, row_block)
    tiled_table = mode_table.reshape(row_count, row_block, point_count)
    own_points = lax.dynamic_slice_in_dim(tiled_table, col_index * point_block, point_block, 2)
    block_part = jnp.einsum(
        "zpsal,slx->zpax",
        lax.all_gather(grouped, "my", axis=3, tiled=True),
        own_points,
        preferred_element_type=jnp.float32,
    ).astype(jnp.bfloat16)
    wave_field = jnp.einsum(
        "zpax,ay->zpxy", block_part, mode_table, preferred_element_type=jnp.float32
    )
    wave_real = wave_field[:, 0]
    wave_imag = wave_field[:, 1]
    density = wave_real * wave_real + wave_imag * wave_imag
    noise_wide = noise_field.astype(jnp.float32)
    drive_term = jnp.stack(
        [
            density * (wave_imag - DAMPING * wave_real) + noise_wide[:, 0],
            density * (-wave_real - DAMPING * wave_imag) + noise_wide[:, 1],
        ],
        1,
    ).astype(jnp.bfloat16)
    proj_columns = jnp.einsum(
        "zpxy,ny->zpnx", drive_term, mode_table, preferred_element_type=jnp.float32
    ).astype(jnp.bfloat16)
    block_part = lax.all_to_all(proj_columns, "my", split_axis=2, concat_axis=3, tiled=True)
    folded = jnp.einsum(
        "zpax,slx->zpsal", block_part, tiled_table, preferred_element_type=jnp.float32
    ).astype(jnp.bfloat16)
    proj_rows = folded.reshape(
        block_part.shape[0], block_part.shape[1], row_count * col_block * row_block
    )
    gathered_rows = lax.all_to_all(proj_rows, "mx", split_axis=2, concat_axis=0, tiled=True)
    slab_back = lax.dynamic_slice_in_dim(mode_table, rep_index * own_block, own_block, 0)[
        :, slab_first : slab_first + planes_all
    ]
    portion = lax.all_gather(gathered_rows, "rep", axis=0, tiled=True)
    plane_grid = portion.reshape(portion.shape[0], 2, col_block, row_block)
    summed = jnp.einsum("zpba,nz->pabn", plane_grid, slab_back, preferred_element_type=jnp.float32)
    return summed.astype(jnp.bfloat16)

def slab_owners(planes, count):
    half = count // 2
    inner = max(1, planes // (2 * count))
    shared = 2 * inner * (half - 1)
    return half, inner, shared, (planes - shared) // 2


def slab_schedule(planes, count, units, rate, first_step):
    half, inner, shared, outer = slab_owners(planes, count)

    def needed(me):
        group = me - half if me >= half else half - 1 - me
        owned = inner if group < half - 1 else outer
        first = group * 2 * inner + (1 if me >= half else 0)
        ready = [first_step + ((k + 1) * units - 1) // rate for k in range(owned)]
        return max(ready[k] + 1 - first - 2 * k for k in range(owned))

    lag_end = max(0, needed(0), needed(count - 1))
    lag_mid = max([lag_end + 1] + [needed(me) for me in range(1, count - 1)])
    return lag_end, lag_mid


def slab_kernel(coef_ref, noise_ref, table_ref, out_ref, back_ref, coef, wide, spread, zmodes, modes, split,
                turned_ref, slab_ref, lines, total, cubic, parts, landed, noise, halves, coef_sem, noise_sem, mode_recv,
                mode_send, sum_recv, sum_send, first_recv, first_send, second_recv, second_send):
    count = lax.axis_size("my")
    me = lax.axis_index("my")
    row_count = lax.axis_size("mx")
    row = lax.axis_index("mx")
    rep_count = lax.axis_size("rep")
    rep = lax.axis_index("rep")
    planes = noise_ref.shape[0]
    planes_rep = planes * row_count
    row_block = coef_ref.shape[1]
    block = coef_ref.shape[2]
    pair = 2 if rep_count % 2 == 0 else 1
    groups = rep_count // pair
    group = lax.div(rep, pair)
    side = lax.rem(rep, pair)
    spots = [(dg, dh) for dg in range(groups) for dh in range(row_count)]
    offsets = [(dr, dh) for dr in range(rep_count) for dh in range(row_count)]
    full = row_block // 128
    rest = row_block % 128
    pieces = zmodes.shape[1]
    mode_count, point_count = table_ref.shape
    point_block = noise_ref.shape[2]
    width = lines.shape[1] // 2
    units = point_count // width
    chunk = max(c for c in (512, 256, 128) if point_count % c == 0)
    rate = max(1, units // 2)
    modes_step, cubic_step = 2, 5
    half, inner, shared, outer = slab_owners(planes, count)
    lag_end, lag_mid = slab_schedule(planes, count, units, rate, cubic_step)
    tail = max(0, planes - 2)
    up = {"my": me + 1}
    down = {"my": me - 1}
    has_up = me < count - 1
    has_down = me > 0

    barrier = pltpu.get_barrier_semaphore()
    line_peers = [(dh, dm) for dh in range(row_count) for dm in range(count)][1:]
    rep_peers = [(dr, dh) for dr, dh in offsets if dr > 0]
    for dh, dm in line_peers:
        pl.semaphore_signal(
            barrier, inc=1,
            device_id={"mx": lax.rem(row + dh, row_count), "my": lax.rem(me + dm, count)},
            device_id_type=MESH,
        )
    for dr, dh in rep_peers:
        pl.semaphore_signal(
            barrier, inc=1,
            device_id={"rep": lax.rem(rep + dr, rep_count), "mx": lax.rem(row + dh, row_count)},
            device_id_type=MESH,
        )

    def rows(j):
        return pl.ds(pl.multiple_of(j * block, block), block)

    def group_of(p):
        return jnp.minimum(lax.div(p, 2 * inner), half - 1)

    def owner_of(p):
        return jnp.where(lax.rem(p, 2) == 1, half + group_of(p), half - 1 - group_of(p))

    def slot_of(p):
        return lax.div(p - group_of(p) * (2 * inner), 2)

    own_group = jnp.where(me >= half, me - half, half - 1 - me)
    owned = jnp.where(own_group < half - 1, inner, outer)

    def plane_of(k):
        return own_group * (2 * inner) + 2 * k + (me >= half).astype(jnp.int32)

    def mode_copy(p, h, j, target_row, target):
        return pltpu.make_async_remote_copy(
            src_ref=zmodes.at[target_row * planes + p],
            dst_ref=modes.at[slot_of(p), h, :, rows(j)],
            send_sem=mode_send.at[p, target_row],
            recv_sem=mode_recv.at[slot_of(p), h, j],
            device_id={"mx": target_row, "my": target},
            device_id_type=MESH,
        )

    def mode_keep(p):
        return pltpu.make_async_copy(
            zmodes.at[row * planes + p], modes.at[slot_of(p), row, :, rows(me)],
            mode_recv.at[slot_of(p), row, me],
        )

    def plane_at(from_group, from_side, from_row, p):
        return ((from_group * pair + from_side) * row_count + from_row) * planes + p

    def first_copy(p, at, received):
        dg, dh = spots[at]
        target_row = lax.rem(row + dh, row_count)
        if at == 0:
            return pltpu.make_async_copy(
                halves.at[p, row], out_ref.at[plane_at(group, side, row, p)], first_send.at[p, 0]
            )
        if received:
            plane = plane_at(
                lax.rem(group + groups - dg, groups), side, lax.rem(row + row_count - dh, row_count), p
            )
        else:
            plane = plane_at(group, side, row, p)
        return pltpu.make_async_remote_copy(
            src_ref=halves.at[p, target_row],
            dst_ref=out_ref.at[plane],
            send_sem=first_send.at[p, at],
            recv_sem=first_recv.at[p, at],
            device_id={"rep": lax.rem(group + dg, groups) * pair + side, "mx": target_row},
            device_id_type=MESH,
        )

    def second_copy(p, at, received):
        dg, dh = spots[at]
        plane = plane_at(
            lax.rem(group + groups - dg, groups), 1 - side if received else side,
            lax.rem(row + row_count - dh, row_count), p,
        )
        return pltpu.make_async_remote_copy(
            src_ref=halves.at[p, row] if at == 0 else out_ref.at[plane],
            dst_ref=out_ref.at[plane],
            send_sem=second_send.at[p, at],
            recv_sem=second_recv.at[p, at],
            device_id={"rep": group * pair + 1 - side},
            device_id_type=MESH,
        )

    def noise_copy(p):
        slot = lax.rem(p, 2)
        return pltpu.make_async_copy(noise_ref.at[p], noise.at[slot], noise_sem.at[slot])

    def sum_copy(p, j, way, slot):
        return pltpu.make_async_remote_copy(
            src_ref=parts.at[p, :, rows(j)],
            dst_ref=landed.at[p, slot],
            send_sem=sum_send.at[p, way, j],
            recv_sem=sum_recv.at[p, slot],
            device_id=down if way else up,
            device_id_type=MESH,
        )

    strips = block // 16

    def coef_copy(i, part):
        strip = pl.ds(pl.multiple_of(i * 16, 16), 16)
        return pltpu.make_async_copy(coef_ref.at[part, :, strip], coef.at[part], coef_sem.at[part])

    noise_copy(0).start()
    if planes > 1:
        noise_copy(1).start()
    coef_copy(0, 0).start()
    coef_copy(0, 1).start()

    def selected(source, offset, wanted):
        shape = (source.shape[1], 128)
        source_at = lax.broadcasted_iota(jnp.int32, shape, 0)
        target_at = lax.broadcasted_iota(jnp.int32, shape, 1)
        chosen = jnp.logical_and(source_at == target_at + offset, target_at < wanted)
        return jnp.dot(
            source, chosen.astype(jnp.float32).astype(jnp.bfloat16), preferred_element_type=jnp.float32
        ).astype(jnp.bfloat16)

    planes_all = planes_rep * rep_count
    slab_first = point_count // 2 - planes_all // 2
    base = slab_first // 128 * 128
    window = slice(base, pl.cdiv(slab_first + planes_all, 128) * 128)

    def prepare_tables():
        own_block = mode_count // rep_count
        own_rows = pl.ds(pl.multiple_of(rep * own_block, own_block), own_block)
        back = selected(table_ref[own_rows, window], slab_first - base, planes_all)
        back_ref[...] = jnp.concatenate([back, jnp.zeros((128 - own_block, 128), jnp.bfloat16)], 0)
        for first in range(0, point_count, 128):
            turned_ref[first : first + 128] = table_ref[:, first : first + 128].T
        split[...] = jnp.zeros_like(split)
        for h in range(row_count):
            for part in range(2):
                for t in range(full + (1 if rest else 0)):
                    size = min(128, row_block - t * 128)
                    source = h * row_block + t * 128
                    place = (h * (full + (1 if rest else 0)) + t) * 128 + (part * rest if size < 128 else 0)
                    split[part, place : place + size] = table_ref[source : source + size]

    def contract_strip(i, carry):
        strip = pl.ds(pl.multiple_of(i * 16, 16), 16)
        for part in range(2):
            coef_copy(i, part).wait()
            wide[part] = jnp.dot(
                coef[part].reshape(row_block * 16, coef.shape[3]), slab_ref[...],
                preferred_element_type=jnp.float32,
            )

            @pl.when(i + 1 < strips)
            def _():
                coef_copy(i + 1, part).start()

        for b in range(16):
            for part in range(2):
                for t in range(full):
                    turn = wide[part, pl.ds(t * 2048 + b, 128, stride=16), :].T[:planes_rep]
                    spread[part * full + t, pl.ds(b, planes_rep, stride=16), :] = turn
            if rest:
                both = [wide[part, pl.ds(full * 2048 + b, rest, stride=16), :] for part in range(2)]
                spread[2 * full, pl.ds(b, planes_rep, stride=16), :] = jnp.concatenate(both, 0).T[:planes_rep]
        for t in range(pieces):
            zmodes[:, t, strip, :] = spread[t].reshape(planes_rep, 16, 128).astype(jnp.bfloat16)
        return carry

    def send_modes(i, carry):
        turn = lax.div(i, 2)
        even = min(shared, planes - shared) // 2
        later = turn - even + (0 if shared > planes - shared else shared // 2)
        mixed = lax.div(turn, 2) + (1 - lax.rem(turn, 2)) * (shared // 2)
        p = 2 * jnp.where(turn < 2 * even, mixed, later) + lax.rem(i, 2)
        target = owner_of(p)
        for dh in range(row_count):
            target_row = lax.rem(row + dh, row_count)
            if dh:
                mode_copy(p, row, me, target_row, target).start()
            else:
                @pl.when(target != me)
                def _():
                    mode_copy(p, row, me, target_row, target).start()

                @pl.when(target == me)
                def _():
                    mode_keep(p).start()
        return carry

    def inside(p):
        return jnp.logical_and(p >= 0, p < planes)

    def span_of(i):
        low = jnp.where(i == planes - 1, tail, i)
        valid = jnp.logical_and(i >= 0, jnp.logical_or(i < tail, i == planes - 1))
        return low, jnp.where(valid, i + 1, low)

    own_points = pl.ds(pl.multiple_of(me * point_block, point_block), point_block)

    def project_noise(p):
        noise_copy(p).wait()
        slot = lax.rem(p, 2)
        step_of = max(c for c in (512, 256, 128) if point_count % c == 0)
        columns = None
        for first in range(0, point_count, step_of):
            span = slice(first, first + step_of)
            field = noise[slot, :, :, span].reshape(2 * point_block, step_of)
            more = lax.dot_general(table_ref[:, span], field, NT, preferred_element_type=jnp.float32)
            columns = more if columns is None else columns + more
        own_table = table_ref[:, own_points]
        for part in range(2):
            column = columns[:, part * point_block : (part + 1) * point_block].astype(jnp.bfloat16)
            parts[p, part] = lax.dot_general(
                column, own_table, NT, preferred_element_type=jnp.float32
            ).astype(jnp.bfloat16)

        @pl.when(p + 2 < planes)
        def _():
            noise_copy(p + 2).start()

    def wait_modes(k):
        p = plane_of(k)
        for h in range(row_count):
            for j in range(count):
                mine = jnp.logical_and(row == h, me == j)

                @pl.when(mine)
                def _():
                    mode_keep(p).wait()

                @pl.when(jnp.logical_not(mine))
                def _():
                    mode_copy(p, h, j, row, me).wait_recv()

    def cubic_unit(u, carry):
        k = lax.div(u, units)
        at = lax.rem(u, units)

        @pl.when(at == 0)
        def _():
            wait_modes(k)

        span = pl.ds(pl.multiple_of(at * width, width), width)
        for part in range(2):
            field = []
            for h in range(row_count):
                field += [modes[k, h, part * full + t] for t in range(full)]
                if rest:
                    field.append(modes[k, h, 2 * full])
            line = jnp.dot(
                jnp.concatenate(field, 1), split[part, :, span], preferred_element_type=jnp.float32
            )
            lines[:, part * width : (part + 1) * width] = line.astype(jnp.bfloat16)
        columns = None
        for first in range(0, point_count, chunk):
            wave = jnp.dot(
                turned_ref[first : first + chunk], lines[...], preferred_element_type=jnp.float32
            )
            wave_real, wave_imag = wave[:, :width], wave[:, width:]
            density = wave_real * wave_real + wave_imag * wave_imag
            drive = jnp.concatenate(
                [
                    (density * (wave_imag - DAMPING * wave_real)).astype(jnp.bfloat16),
                    (density * (-wave_real - DAMPING * wave_imag)).astype(jnp.bfloat16),
                ],
                1,
            )
            more = jnp.dot(
                table_ref[:, first : first + chunk], drive, preferred_element_type=jnp.float32
            )
            columns = more if columns is None else columns + more
        for part in range(2):
            more = jnp.dot(
                columns[:, part * width : (part + 1) * width].astype(jnp.bfloat16),
                turned_ref[span], preferred_element_type=jnp.float32,
            )

            @pl.when(at == 0)
            def _():
                total[part] = more

            @pl.when(at > 0)
            def _():
                total[part] += more

        @pl.when(at == units - 1)
        def _():
            cubic[k] = total[...].astype(jnp.bfloat16)

        return carry

    def add(p, j, slot):
        both = parts[p, :, rows(j)].astype(jnp.float32) + landed[p, slot].astype(jnp.float32)
        parts[p, :, rows(j)] = both.astype(jnp.bfloat16)

    rise_lag = jnp.where(me == 0, lag_end, lag_mid + me - 1)
    sink_lag = jnp.where(me == count - 1, lag_end, lag_mid + count - 2 - me)
    merge_lag = jnp.minimum(rise_lag, sink_lag)
    done_lag = jnp.maximum(rise_lag, sink_lag)

    def step(s, carry):
        sent = jnp.where(s < shared, s, s - lag_end)
        at_end = jnp.logical_or(me == 0, me == count - 1)
        merging = jnp.where(at_end, sent, s - merge_lag)

        @pl.when(jnp.logical_and(inside(merging), owner_of(merging) == me))
        def _():
            both = parts[merging].astype(jnp.float32) + cubic[slot_of(merging)].astype(jnp.float32)
            parts[merging] = both.astype(jnp.bfloat16)

        low, high = span_of(sent)
        high = jnp.where(jnp.logical_or(s < shared, sent >= shared), high, low)

        @pl.when(me == 0)
        def _():
            for j in range(count - 1, 0, -1):
                def emit(p, carry):
                    sum_copy(p, j, 0, j).start()
                    return carry

                lax.fori_loop(low, high, emit, 0)

        @pl.when(me == count - 1)
        def _():
            for j in range(count - 1):
                def emit(p, carry):
                    sum_copy(p, j, 1, count if j == count - 2 else j).start()
                    return carry

                lax.fori_loop(low, high, emit, 0)

        @pl.when(s == modes_step)
        def _():
            slab_ref[...] = selected(
                table_ref[:, window], slab_first - base + rep * planes_rep, planes_rep
            )
            lax.fori_loop(0, strips, contract_strip, 0)
            lax.fori_loop(0, planes, send_modes, 0)
            prepare_tables()

        @pl.when(s + 1 < planes)
        def _():
            project_noise(s + 1)

        unit = (s - cubic_step) * rate
        lax.fori_loop(
            jnp.clip(unit, 0, owned * units), jnp.clip(unit + rate, 0, owned * units), cubic_unit, 0
        )

        low, high = span_of(s - rise_lag)
        for far in range(count - 2, 0, -1):
            @pl.when(jnp.logical_and(has_down, me + far <= count - 1))
            def _():
                j = me + far

                def relay(p, carry):
                    sum_copy(p, j, 0, j).wait_recv()
                    add(p, j, j)
                    sum_copy(p, j, 0, j).start()
                    return carry

                lax.fori_loop(low, high, relay, 0)

        low, high = span_of(s - sink_lag)
        for far in range(count - 2, 0, -1):
            @pl.when(jnp.logical_and(has_up, me - far >= 0))
            def _():
                j = me - far

                def relay(p, carry):
                    sum_copy(p, j, 1, j).wait_recv()
                    add(p, j, j)
                    sum_copy(p, j, 1, count if far == 1 else j).start()
                    return carry

                lax.fori_loop(low, high, relay, 0)

        def finish_plane(p, carry):
            @pl.when(has_down)
            def _():
                sum_copy(p, me, 0, me).wait_recv()
                add(p, me, me)

            @pl.when(has_up)
            def _():
                sum_copy(p, me, 1, count).wait_recv()
                add(p, me, count)

            whole = [parts[p, part, rows(me)] for part in range(2)]
            for h in range(row_count):
                for part in range(2):
                    for t in range(full):
                        place = h * row_block + t * 128
                        halves[p, h, part * full + t] = whole[part][:, place : place + 128]
                if rest:
                    place = h * row_block + full * 128
                    halves[p, h, 2 * full] = jnp.concatenate(
                        [whole[part][:, place : place + rest] for part in range(2)], 1
                    )
            for at in range(len(spots) - 1, -1, -1):
                first_copy(p, at, False).start()
            if pair == 2:
                second_copy(p, 0, False).start()
            return carry

        low, high = span_of(s - done_lag)
        lax.fori_loop(low, high, finish_plane, 0)

        def pass_on(p, carry):
            for at in range(1, len(spots)):
                first_copy(p, at, True).wait_recv()
                if pair == 2:
                    second_copy(p, at, False).start()
            return carry

        low, high = span_of(s - done_lag - 1)
        lax.fori_loop(low, high, pass_on, 0)
        return carry

    project_noise(0)
    pl.semaphore_wait(barrier, len(line_peers) + len(rep_peers))
    lax.fori_loop(0, planes + lag_mid + count - 1, step, 0)

    def finish(p, carry):
        for j in range(count):
            @pl.when(j > me)
            def _():
                sum_copy(p, j, 0, j).wait_send()

            @pl.when(j < me)
            def _():
                sum_copy(p, j, 1, j).wait_send()

        target = owner_of(p)
        for dh in range(row_count):
            target_row = lax.rem(row + dh, row_count)
            if dh:
                mode_copy(p, row, me, target_row, target).wait_send()
            else:
                @pl.when(target != me)
                def _():
                    mode_copy(p, row, me, target_row, target).wait_send()

        first_copy(p, 0, False).wait()
        for at in range(len(spots)):
            if at:
                first_copy(p, at, False).wait_send()
            if pair == 2:
                second_copy(p, at, False).wait_send()
                second_copy(p, at, True).wait_recv()
        return carry

    lax.fori_loop(0, planes, finish, 0)


def slab_planes(coefficients, noise_field, mode_table):
    count = lax.axis_size("my")
    mode_count = mode_table.shape[0]
    row_count = lax.axis_size("mx")
    rep_count = lax.axis_size("rep")
    _, row_block, block, depth = coefficients.shape
    planes = noise_field.shape[0]
    planes_rep = planes * row_count
    outer = slab_owners(planes, count)[3]
    pieces = 2 * row_block // 128
    places = row_count * pl.cdiv(row_block, 128) * 128
    spots = row_count * (rep_count // (2 if rep_count % 2 == 0 else 1))
    point_block, point_count = noise_field.shape[2:]
    width = max(c for c in (256, 128) if point_count % c == 0)
    vmem = pl.BlockSpec(memory_space=pltpu.VMEM)
    hbm = pl.BlockSpec(memory_space=pl.ANY)
    dma = pltpu.SemaphoreType.DMA
    flops = 12 * planes * mode_count * point_block * (point_count + mode_count)
    return pl.pallas_call(
        slab_kernel,
        out_shape=(
            jax.ShapeDtypeStruct((planes_rep * rep_count, pieces, block, 128), jnp.bfloat16),
            jax.ShapeDtypeStruct((128, 128), jnp.bfloat16),
        ),
        in_specs=[hbm, hbm, vmem],
        out_specs=(hbm, vmem),
        scratch_shapes=[
            pltpu.VMEM((2, row_block, 16, depth), jnp.bfloat16),
            pltpu.VMEM((2, row_block * 16, 128), jnp.float32),
            pltpu.VMEM((pieces, planes_rep * 16, 128), jnp.float32),
            pltpu.VMEM((planes_rep, pieces, block, 128), jnp.bfloat16),
            pltpu.VMEM((outer, row_count, pieces, mode_count, 128), jnp.bfloat16),
            pltpu.VMEM((2, places, point_count), jnp.bfloat16),
            pltpu.VMEM((point_count, mode_count), jnp.bfloat16),
            pltpu.VMEM((depth, 128), jnp.bfloat16),
            pltpu.VMEM((mode_count, 2 * width), jnp.bfloat16),
            pltpu.VMEM((2, mode_count, mode_count), jnp.float32),
            pltpu.VMEM((outer, 2, mode_count, mode_count), jnp.bfloat16),
            pltpu.VMEM((planes, 2, mode_count, mode_count), jnp.bfloat16),
            pltpu.VMEM((planes, count + 1, 2, block, mode_count), jnp.bfloat16),
            pltpu.VMEM((2, 2, point_block, point_count), jnp.bfloat16),
            pltpu.VMEM((planes, row_count, pieces, block, 128), jnp.bfloat16),
            dma((2,)),
            dma((2,)),
            dma((outer, row_count, count)),
            dma((planes, row_count)),
            dma((planes, count + 1)),
            dma((planes, 2, count)),
            dma((planes, spots)),
            dma((planes, spots)),
            dma((planes, spots)),
            dma((planes, spots)),
        ],
        compiler_params=pltpu.CompilerParams(
            collective_id=0, has_side_effects=True, vmem_limit_bytes=60 * 1024 * 1024
        ),
        cost_estimate=pl.CostEstimate(
            flops=flops, bytes_accessed=noise_field.size * 2, transcendentals=0
        ),
    )(coefficients, noise_field, mode_table)


def update_kernel(grid_ref, slab_ref, out_ref, wide, lines):
    planes, pieces, strip, lanes = grid_ref.shape
    _, row_block, _, own_block = out_ref.shape
    full = row_block // lanes
    rest = row_block % lanes
    for t in range(pieces):
        wide[t] = grid_ref[:, t].astype(jnp.float32).reshape(planes * strip, lanes)
    for t in range(pieces):
        for b in range(0, strip, 2):
            pair = [
                wide[t, pl.ds(b + e, planes, stride=strip), :].astype(jnp.bfloat16) for e in range(2)
            ]
            both = jnp.dot(
                slab_ref[...], jnp.concatenate(pair, 1), preferred_element_type=jnp.float32
            )
            for e in range(2):
                turn = both[:, e * lanes : (e + 1) * lanes].T
                if t < 2 * full:
                    first = (t % full) * lanes * strip + b + e
                    lines[t // full, pl.ds(first, lanes, stride=strip), :] = turn
                else:
                    first = full * lanes * strip + b + e
                    for part in range(2):
                        lines[part, pl.ds(first, rest, stride=strip), :] = turn[
                            part * rest : (part + 1) * rest
                        ]
    for part in range(2):
        out_ref[part] = (
            lines[part, :, :own_block].reshape(row_block, strip, own_block).astype(jnp.bfloat16)
        )


def update_planes(plane_grid, slab_back, row_block, own_block):
    planes, pieces, block, lanes = plane_grid.shape
    strip = 16
    return pl.pallas_call(
        update_kernel,
        grid=(block // strip,),
        out_shape=jax.ShapeDtypeStruct((2, row_block, block, own_block), jnp.bfloat16),
        in_specs=[
            pl.BlockSpec((planes, pieces, strip, lanes), lambda b: (0, 0, b, 0)),
            pl.BlockSpec((lanes, planes), lambda b: (0, 0)),
        ],
        out_specs=pl.BlockSpec((2, row_block, strip, own_block), lambda b: (0, 0, b, 0)),
        scratch_shapes=[
            pltpu.VMEM((pieces, planes * strip, lanes), jnp.float32),
            pltpu.VMEM((2, row_block * strip, lanes), jnp.float32),
        ],
        compiler_params=pltpu.CompilerParams(vmem_limit_bytes=60 * 1024 * 1024),
        cost_estimate=pl.CostEstimate(
            flops=4 * planes * row_block * block * own_block, bytes_accessed=plane_grid.size * 2,
            transcendentals=0,
        ),
    )(plane_grid, slab_back)


def body(coefficients, noise_field, mode_table):
    rep_count = lax.axis_size("rep")
    row_count = lax.axis_size("mx")
    col_count = lax.axis_size("my")
    planes_dev = noise_field.shape[0]
    planes_rep = planes_dev * row_count
    planes_all = planes_rep * rep_count
    mode_count = mode_table.shape[0]
    point_count = mode_table.shape[1]
    row_block = mode_count // row_count
    col_block = mode_count // col_count
    point_block = point_count // col_count
    own_block = mode_count // rep_count
    if (
        col_block % 16 or row_block % 16 or point_block % 128 or mode_count % 128
        or row_block % 64 or col_count < 2 or col_count % 2 or planes_dev % (2 * col_count)
        or planes_rep % 8 or planes_all != 128 or own_block > 128 or own_block % 16
    ):
        return plain_body(coefficients, noise_field, mode_table)
    plane_grid, slab_back = slab_planes(coefficients, noise_field, mode_table)
    return update_planes(plane_grid, slab_back, row_block, own_block)


def solution(mesh):
    in_specs = (P(None, "mx", "my", None), P(("rep", "mx"), None, "my", None), P())
    out_specs = P(None, "mx", "my", "rep")
    return jax.shard_map(body, mesh=mesh, in_specs=in_specs, out_specs=out_specs, check_vma=False)
```
